32 devices in a mesh: row: 4 (over z), col: 8 (over y, x, core).
Axes of the slice: x: 2, y: 2, z: 4, core: 2. Of those that a mesh axis runs over, the one named last changes fastest.
Arguments:
- latent: float32 [2, 1024, 2048], P(None, 'row', 'col'), may hold values from -3 to 3
- momentum: float32 [2, 1024, 2048], P(None, 'row', 'col'), may hold values from -4 to 4
- hyper_params: float32 [2, 2], replicated, may hold values from 0.3 to 0.7
- velocity: float32 [2, 2], replicated, may hold values from -3 to 3
- step_size: float32 [2], replicated, may hold values from 0.08 to 0.12
- counts: int32 [1024, 2048], P('row', 'col'), may hold values from 0 to 7
- kappa_field: float32 [1024, 2048], P('row', 'col'), may hold values from 0.1 to 1
Outputs:
- latent_out: float32 [2, 1024, 2048], P(None, 'row', 'col')
- momentum_out: float32 [2, 1024, 2048], P(None, 'row', 'col')
- hyper_out: float32 [2, 2], replicated
- velocity_out: float32 [2, 2], replicated
The draws below stay inside these ranges and needn't reach their ends.
All inputs are finite; a program needn't handle non-finite values.
Results may differ from the reference program's by a relative error of at most 0.0001.
Values sent between devices are 32-bit elements; how exact they have to be, the bound alone decides.
A program may use at most 64 MiB of HBM per device.

```python
import math
import jax
import jax.numpy as jnp
from jax import lax

CHAINS = 2
STEPS = 10
NR = 1024
NC = 2048


def draw_latent(key, part):
    values = jax.random.uniform(key, (CHAINS, NR, NC), jnp.float32, -3.0, 3.0)
    return values


def draw_counts(key, part):
    columns = jnp.arange(NC, dtype=jnp.int32)
    ceiling = jnp.broadcast_to(3 + 6 * columns // NC, (NR, NC))
    return jax.random.randint(key, (NR, NC), 0, ceiling, dtype=jnp.int32)


def levels(stream_key, extent, cuts, low, high):
    level = 1.0
    for position, blocks in cuts:
        draws = jax.random.uniform(jax.random.fold_in(jax.random.fold_in(stream_key, 6), position), (blocks,), jnp.float32, low / len(cuts), high / len(cuts))
        level = level * jnp.repeat(jnp.exp(draws), extent[position] // blocks).reshape((-1,) + (1,) * (len(extent) - 1 - position))
    return level


def bell_draw(rng, extent, scale, bound, held_as=jnp.bfloat16):
    array = jax.random.normal(rng, extent, jnp.float32) * scale
    return jnp.minimum(jnp.maximum(array, -bound), bound).astype(held_as)


def setup_inputs(seed: int = 0) -> dict:
    seeds = jax.random.split(jax.random.key(seed), 8)
    latent = draw_latent(jax.random.fold_in(seeds[7], 71), 0)
    momentum = jnp.clip(jax.random.uniform(seeds[1], (CHAINS, NR, NC), jnp.float32, -4.0, 4.0) * levels(seeds[1], (CHAINS, NR, NC), ((1, 4), (2, 8)), -0.4, 0.0), -4.0, 4.0)
    hyper_params = jnp.clip(jax.random.uniform(seeds[2], (2, CHAINS), jnp.float32, 0.3, 0.7), 0.3, 0.7)
    velocity = bell_draw(seeds[3], (2, CHAINS), 0.3, 3.0, jnp.float32)
    step_size = jnp.clip(jnp.exp(jax.random.uniform(seeds[4], (CHAINS,), jnp.float32, math.log(0.08), math.log(0.12))), 0.08, 0.12)
    counts = draw_counts(jax.random.fold_in(seeds[7], 71), 0)
    kappa_field = jnp.clip(jnp.exp(math.log(1.0) - 2.3025851 * jax.random.uniform(seeds[6], (NR, NC), jnp.float32) ** levels(seeds[6], (NR, NC), ((0, 4), (1, 8)), -0.2, 0.2)), 0.1, 1.0)
    return {"latent": latent, "momentum": momentum, "hyper_params": hyper_params, "velocity": velocity, "step_size": step_size, "counts": counts, "kappa_field": kappa_field}


def stencil(field):
    return jnp.roll(field, 1, 0) + jnp.roll(field, -1, 0) + jnp.roll(field, 1, 1) + jnp.roll(field, -1, 1)


def reference(latent, momentum, hyper_params, velocity, step_size, counts, kappa_field):
    count_float = counts.astype(jnp.float32)
    total = float(NR * NC)

    def gradient_at(field, params):
        tau_value = jnp.exp(params[1])
        applied = (kappa_field + 4.0) * field - stencil(field)
        intensity = jnp.exp(params[0] + field)
        gradient = tau_value * applied - count_float + intensity
        quadratic = jnp.sum(field * applied)
        excess = jnp.sum(intensity - count_float)
        accel = jnp.stack([excess / total, 0.5 * tau_value * quadratic / total - 0.5])
        return gradient, accel

    def single_chain(inputs):
        field, moment, params, speed, size_value = inputs
        gradient, accel = gradient_at(field, params)
        for index_step in range(STEPS):
            moment = moment - 0.5 * size_value * gradient
            speed = speed - 0.5 * size_value * accel
            field = field + size_value * moment
            params = params + size_value * speed
            gradient, accel = gradient_at(field, params)
            moment = moment - 0.5 * size_value * gradient
            speed = speed - 0.5 * size_value * accel
        return field, moment, params, speed

    results = lax.map(single_chain, (latent, momentum, hyper_params.T, velocity.T, step_size))
    return results[0], results[1], results[2].T, results[3].T
```

```python
import functools

import jax
import jax.numpy as jnp
from jax import lax
from jax.experimental import pallas as pl
from jax.experimental.pallas import tpu as pltpu
from jax.sharding import PartitionSpec as P

STEPS = 10
HALO = 16
EDGE = 8
PAD = 8
TOP = PAD + HALO
LANES = 128
SEG = 16
MESH = pl.DeviceIdType.MESH
COEFS = 6


def signal_rounds(nr, nc):
    rounds, reach = [], 1
    while reach < nr // 2 or reach < nc // 2:
        rs = (0, reach, -reach) if reach < nr // 2 else (0,)
        cs = (0, reach, -reach) if reach < nc // 2 else (0,)
        rounds.append([(r, c) for r in rs for c in cs if (r, c) != (0, 0)])
        reach *= 2
    return rounds


def kernel(
    sizes, latent, momentum, counts, kappa, hyper_in, velocity_in, step_in,
    latent_out, momentum_out, hyper_out, velocity_out,
    state, field_u, diagonal, applied, intensity, scaled, scaled_applied, fresh, raw_counts,
    pack_one, pack_two, take_one, take_two, corner_one, corner_two,
    payload, gathered, scal, hyper, velocity, step_size,
    load_sem, halo_send, halo_recv, sum_send, sum_recv, round_sem,
):
    nr, nc, chains, rows, tiles, total = sizes
    devices = nr * nc
    row, col = lax.axis_index("row"), lax.axis_index("col")
    me = row * nc + col
    kap, cnt = 2 * chains, 2 * chains + 1
    fold_one, fold_two = LANES // (SEG * chains), LANES // (SEG * (chains + 2))
    rows_one, rows_two = rows // fold_one, rows // fold_two
    own = pl.ds(TOP, rows)
    everything = range(tiles + 1)

    smalls = [(hyper_in, hyper), (velocity_in, velocity), (step_in, step_size)]
    vloads, loads = [], []
    for c in range(chains):
        for j in range(tiles):
            cols = pl.ds(j * LANES, LANES)
            vloads.append((latent.at[c, :, cols], state.at[c, j, own, :]))
            loads.append((momentum.at[c, :, cols], state.at[chains + c, j, own, :]))
    for j in range(tiles):
        cols = pl.ds(j * LANES, LANES)
        loads.append((kappa.at[:, cols], state.at[kap, j, own, :]))
        loads.append((counts.at[:, cols], raw_counts.at[j]))
    first_loads = len(vloads)
    loads = [
        pltpu.make_async_copy(s, d, load_sem.at[i]) for i, (s, d) in enumerate(vloads + loads + smalls)
    ]
    for copy in loads:
        copy.start()

    def at(dr, dc):
        return (lax.rem(row + (dr + nr), nr), lax.rem(col + (dc + nc), nc))

    near = [(r, c) for r in (0, 1, -1) for c in (0, 1, -1) if (r, c) != (0, 0)]
    barrier = pltpu.get_barrier_semaphore()
    for r, c in near:
        pl.semaphore_signal(barrier, inc=1, device_id=at(r, c), device_id_type=MESH)

    lane = lax.broadcasted_iota(jnp.int32, (8, LANES), 1)
    sublane = lax.broadcasted_iota(jnp.int32, (8, LANES), 0)
    lane_row = lax.broadcasted_iota(jnp.int32, (1, LANES), 1)
    seg = lane_row // SEG
    first, last = lane_row == 0, lane_row == LANES - 1

    def fold(x):
        return sum(x[8 * i : 8 * i + 8] for i in range(x.shape[0] // 8))

    def whole(x):
        return jnp.broadcast_to(jnp.sum(jnp.sum(x, axis=0, keepdims=True), axis=1, keepdims=True), (8, LANES))

    def pack(ref, arrays, depth, folds):
        heads = tails = None
        for s in range(folds):
            part = pl.ds(TOP + s * depth, depth)
            for i, a in enumerate(arrays):
                slot = s * len(arrays) + i
                head, tail = state[a, 0, part, :], state[a, tiles - 1, part, :]
                if slot:
                    head = pltpu.roll(head, slot * SEG, 1)
                tail = pltpu.roll(tail, (slot + 1) * SEG % LANES, 1) if (slot + 1) * SEG % LANES else tail
                heads = head if heads is None else jnp.where(seg == slot, head, heads)
                tails = tail if tails is None else jnp.where(seg == slot, tail, tails)
        ref[0] = heads
        ref[1] = tails

    def unpack(right, left, slot_right, slot_left):
        turn = (LANES - SEG * slot_right) % LANES
        right = pltpu.roll(right, turn, 1) if turn else right
        turn = (LANES - SEG - SEG * slot_left) % LANES
        left = pltpu.roll(left, turn, 1) if turn else left
        return jnp.where(seg == 0, right, jnp.where(seg == LANES // SEG - 1, left, 0.0))

    for copy in loads[:first_loads]:
        copy.wait()
    pack(pack_one, list(range(chains)), rows_one, fold_one)
    pl.semaphore_wait(barrier, len(near))

    remotes = []

    def remote(src, dst, where):
        copy = pltpu.make_async_remote_copy(
            src_ref=src, dst_ref=dst, send_sem=halo_send.at[len(remotes)], recv_sem=halo_recv.at[len(remotes)],
            device_id=where, device_id_type=MESH,
        )
        remotes.append(copy)
        copy.start()

    vs, rest = pl.ds(0, chains), pl.ds(chains, chains + 2)
    flat = pl.ds(0, tiles)

    def rowcopies(arrays, near_row, depth):
        remote(
            state.at[arrays, flat, pl.ds(TOP + near_row, depth), :],
            state.at[arrays, flat, pl.ds(TOP + rows + near_row, depth), :],
            at(-1, 0),
        )
        remote(
            state.at[arrays, flat, pl.ds(TOP + rows - near_row - depth, depth), :],
            state.at[arrays, flat, pl.ds(TOP - near_row - depth, depth), :],
            at(1, 0),
        )

    remote(pack_one.at[0], take_one.at[0], at(0, -1))
    remote(pack_one.at[1], take_one.at[1], at(0, 1))
    rowcopies(vs, 0, EDGE)
    stage_one = len(remotes)

    rounds = signal_rounds(nr, nc)

    def tell(i):
        for r, c in rounds[i]:
            pl.semaphore_signal(round_sem.at[i], inc=1, device_id=at(r, c), device_id_type=MESH)

    tell(0)

    for copy in loads[first_loads:]:
        copy.wait()
    counted = jnp.zeros((8, LANES), jnp.float32)
    for j in range(tiles):
        value = raw_counts[j].astype(jnp.float32)
        state[cnt, j, own, :] = value
        counted += fold(value)
    pack(pack_two, list(range(chains, 2 * chains + 2)), rows_two, fold_two)
    rowcopies(vs, EDGE, HALO - EDGE)
    remote(pack_two.at[0], take_two.at[0], at(0, -1))
    remote(pack_two.at[1], take_two.at[1], at(0, 1))
    rowcopies(rest, 0, HALO)
    for side, dc in ((0, -1), (1, 1)):
        for vert, dr in ((1, -1), (0, 1)):
            for mine, theirs, deep in ((pack_one, corner_one, rows_one), (pack_two, corner_two, rows_two)):
                start = 0 if vert else deep - HALO
                remote(mine.at[side, pl.ds(start, HALO)], theirs.at[side, vert], at(dr, dc))

    h = [step_size[c] for c in range(chains)]
    hh = [h[c] * h[c] for c in range(chains)]

    def full(value):
        return jnp.full((8, LANES), value, jnp.float32)

    TAU, EXO, HYQ, HYE, VEQ, VEE = (i * chains for i in range(6))
    CO = 6 * chains
    LOCAL = CO + COEFS * chains
    for c in range(chains):
        scal[HYQ + c] = full(hyper[1, c])
        scal[HYE + c] = full(hyper[0, c])
        scal[VEQ + c] = full(velocity[1, c])
        scal[VEE + c] = full(velocity[0, c])
        scal[TAU + c] = jnp.exp(full(hyper[1, c]))
        scal[EXO + c] = jnp.exp(full(hyper[0, c]))
    scal[LOCAL] = whole(counted)

    mass = []
    for c in range(chains):
        acc = None
        for j in range(tiles):
            value = jnp.exp(state[c, j, own, :])
            intensity[c, j, own, :] = value
            acc = fold(value) if acc is None else acc + fold(value)
        mass.append(whole(acc))
    for j in range(tiles):
        diagonal[j, own, :] = state[kap, j, own, :] + 4.0
        for c in range(chains):
            hc = hh[c] * state[cnt, j, own, :]
            scaled[c, j, own, :] = hc
            field_u[c, j, own, :] = state[c, j, own, :] + (h[c] * state[chains + c, j, own, :] + 0.5 * hc)

    def stencil(ref, c, r, deep, lane_tiles):
        rowset = pl.ds(r, deep)
        at_tile = [ref[c, j, rowset, :] for j in everything]
        n = tiles + 1
        used = sorted({(j + s) % n for j in lane_tiles for s in (-1, 0)})
        to_right = {j: pltpu.roll(at_tile[j], 1, 1) for j in used}
        used = sorted({(j + s) % n for j in lane_tiles for s in (1, 0)})
        to_left = {j: pltpu.roll(at_tile[j], LANES - 1, 1) for j in used}
        out = []
        for j in lane_tiles:
            beside = jnp.where(first, to_right[(j - 1) % n], to_right[j])
            beside += jnp.where(last, to_left[(j + 1) % n], to_left[j])
            beside += ref[c, j, pl.ds(r - 1, deep), :] + ref[c, j, pl.ds(r + 1, deep), :]
            out.append((j, at_tile[j], diagonal[j, rowset, :] * at_tile[j] - beside))
        return out

    DEEP = 64

    def own_blocks():
        return [TOP + i * DEEP for i in range(rows // DEEP)]

    def sides():
        out = [(TOP + i * DEEP, DEEP, [tiles]) for i in range(rows // DEEP)]
        return out + [(PAD, HALO, everything), (TOP + rows, HALO, everything)]

    def own_applied():
        quads = []
        for c in range(chains):
            acc = jnp.zeros((8, LANES), jnp.float32)
            for r in own_blocks():
                for j, v, av in stencil(state, c, r, DEEP, range(tiles)):
                    applied[c, j, pl.ds(r, DEEP), :] = av
                    acc += fold(v * av)
            quads.append(acc)
        return [whole(q) for q in quads]

    def halo_applied():
        for c in range(chains):
            for r, deep, lane_tiles in sides():
                for j, _, av in stencil(state, c, r, deep, lane_tiles):
                    applied[c, j, pl.ds(r, deep), :] = av

    others = sorted(range(1, devices), key=lambda d: -min(d, devices - d))

    def peer(d):
        other = lax.rem(me + d, devices)
        return (other // nc, lax.rem(other, nc))

    def send(k, quad, mass):
        out = scal[LOCAL][:1]
        for i, value in enumerate(quad + mass):
            out = jnp.where(seg == i, value[:1], out)
        payload[k] = out
        gathered[k, me] = out
        for d in others:
            pltpu.make_async_remote_copy(
                src_ref=payload.at[k], dst_ref=gathered.at[k, me],
                send_sem=sum_send.at[k], recv_sem=sum_recv.at[k],
                device_id=peer(d), device_id_type=MESH,
            ).start()

    def bulk(k):
        ref = gathered.at[k, pl.ds(0, devices - 1)]
        return pltpu.make_async_remote_copy(
            src_ref=ref, dst_ref=ref, send_sem=sum_send.at[k], recv_sem=sum_recv.at[k],
            device_id=peer(1), device_id_type=MESH,
        )

    def collect(k):
        bulk(k).wait_recv()
        summed = jnp.broadcast_to(jnp.sum(gathered[k], axis=0), (8, LANES))
        values = [
            jnp.broadcast_to(jnp.sum(jnp.where(lane == i * SEG, summed, 0.0), axis=1, keepdims=True), (8, LANES))
            for i in range(2 * chains + 1)
        ]
        return values[:chains], values[chains : 2 * chains], values[2 * chains]

    def kick_hyper(k, part):
        quad, mass, number = collect(k)
        for c in range(chains):
            aq = (0.5 / total) * (scal[TAU + c] * quad[c]) - 0.5
            ae = (scal[EXO + c] * mass[c] - number) * (1.0 / total)
            scal[VEQ + c] = scal[VEQ + c] - (part * h[c]) * aq
            scal[VEE + c] = scal[VEE + c] - (part * h[c]) * ae

    def drift_hyper():
        for c in range(chains):
            q = scal[HYQ + c] + h[c] * scal[VEQ + c]
            e = scal[HYE + c] + h[c] * scal[VEE + c]
            scal[HYQ + c] = q
            scal[HYE + c] = e
            scal[TAU + c] = jnp.exp(q)
            scal[EXO + c] = jnp.exp(e)

    def weights(part):
        xs = [(part * hh[c]) * scal[TAU + c] for c in range(chains)]
        ys = [(part * hh[c]) * scal[EXO + c] for c in range(chains)]
        return xs, ys

    def own_fresh(xs, ys):
        out = []
        for c in range(chains):
            x, y = xs[c][:1], ys[c][:1]
            acc = jnp.zeros((8, LANES), jnp.float32)
            for j in range(tiles):
                v = field_u[c, j, own, :] - x * applied[c, j, own, :] - y * intensity[c, j, own, :]
                value = jnp.exp(v)
                fresh[c, j] = v
                intensity[c, j, own, :] = value
                acc += fold(value)
            out.append(acc)
        return [whole(acc) for acc in out]

    def own_settle():
        for c in range(chains):
            for j in range(tiles):
                v = fresh[c, j]
                field_u[c, j, own, :] = (v + v) - state[c, j, own, :] + scaled[c, j, own, :]
                state[c, j, own, :] = v

    def halo_advance(xs, ys):
        for c in range(chains):
            x, y = xs[c][:1], ys[c][:1]
            for r, deep, lane_tiles in sides():
                rowset = pl.ds(r, deep)
                for j in lane_tiles:
                    v = field_u[c, j, rowset, :] - x * applied[c, j, rowset, :] - y * intensity[c, j, rowset, :]
                    field_u[c, j, rowset, :] = (v + v) - state[c, j, rowset, :] + scaled[c, j, rowset, :]
                    intensity[c, j, rowset, :] = jnp.exp(v)
                    state[c, j, rowset, :] = v

    def own_coefs(direct):
        for c in range(chains):
            sums = [jnp.zeros((8, LANES), jnp.float32)] * COEFS
            if not direct:
                for r in own_blocks():
                    rowset = pl.ds(r, DEEP)
                    for j, v, av in stencil(state, c, r, DEEP, range(tiles)):
                        au = (av + av) - applied[c, j, rowset, :] + scaled_applied[c, j, pl.ds(r - TOP, DEEP), :]
                        applied[c, j, rowset, :] = av
                        sums[0] += fold(field_u[c, j, rowset, :] * au)
                        sums[1] += fold(av * au)
                        sums[2] += fold(intensity[c, j, rowset, :] * au)
            yield c, sums

    def finish_coefs(direct, c, sums):
        for r in own_blocks():
            rowset = pl.ds(r, DEEP)
            if direct:
                for j, u, au in stencil(field_u, c, r, DEEP, range(tiles)):
                    sums[0] += fold(u * au)
                    sums[1] += fold(applied[c, j, rowset, :] * au)
                    sums[2] += fold(intensity[c, j, rowset, :] * au)
            for j, a, aa in stencil(applied, c, r, DEEP, range(tiles)):
                sums[3] += fold(a * aa)
                sums[4] += fold(intensity[c, j, rowset, :] * aa)
            for j, e, ae in stencil(intensity, c, r, DEEP, range(tiles)):
                sums[5] += fold(e * ae)
        for i in range(COEFS):
            scal[CO + COEFS * c + i] = whole(sums[i])

    def predicted(xs, ys):
        out = []
        for c in range(chains):
            k0, k1, k2, k3, k4, k5 = [scal[CO + COEFS * c + i] for i in range(COEFS)]
            x, y = xs[c], ys[c]
            out.append(k0 - 2.0 * (x * k1 + y * k2) + (x * (x * k3 + 2.0 * (y * k4)) + y * (y * k5)))
        return out

    for i in range(len(rounds)):
        pl.semaphore_wait(round_sem.at[i], len(rounds[i]))
        if i + 1 < len(rounds):
            tell(i + 1)
        if i == 0:
            for copy in remotes[:stage_one]:
                copy.wait_recv()
            for c in range(chains):
                for s in range(fold_one):
                    slot = s * chains + c
                    state[c, tiles, pl.ds(TOP + s * rows_one, rows_one), :] = unpack(
                        take_one[0], take_one[1], slot, slot
                    )
            quad = own_applied()
    send(0, quad, mass)

    xs, ys = weights(0.5)
    mass = own_fresh(xs, ys)

    for copy in remotes[stage_one:]:
        copy.wait_recv()
    for copy in remotes:
        copy.wait_send()

    strips = [(TOP + s * rows_two, rows_two, take_two.at[0], take_two.at[1], s, s) for s in range(fold_two)]
    strips += [
        (PAD, HALO, corner_two.at[0, 0], corner_two.at[1, 0], fold_two - 1, fold_two - 1),
        (TOP + rows, HALO, corner_two.at[0, 1], corner_two.at[1, 1], 0, 0),
    ]
    for r, deep, right, left, sr, sl in strips:
        for i in range(chains + 2):
            value = unpack(right[...], left[...], sr * (chains + 2) + i, sl * (chains + 2) + i)
            state[chains + i, tiles, pl.ds(r, deep), :] = value
    for vert, r, s in ((0, PAD, fold_one - 1), (1, TOP + rows, 0)):
        for c in range(chains):
            state[c, tiles, pl.ds(r, HALO), :] = unpack(
                corner_one[0, vert], corner_one[1, vert], s * chains + c, s * chains + c
            )
    for r, deep, lane_tiles in sides():
        rowset = pl.ds(r, deep)
        for j in lane_tiles:
            diagonal[j, rowset, :] = state[kap, j, rowset, :] + 4.0
            for c in range(chains):
                hc = hh[c] * state[cnt, j, rowset, :]
                scaled[c, j, rowset, :] = hc
                v = state[c, j, rowset, :]
                intensity[c, j, rowset, :] = jnp.exp(v)
                field_u[c, j, rowset, :] = v + (h[c] * state[chains + c, j, rowset, :] + 0.5 * hc)
    halo_applied()
    halo_advance(xs, ys)
    own_settle()
    send(1, own_applied(), mass)
    halo_applied()
    for r in own_blocks():
        for j, _, value in stencil(state, cnt, r, DEEP, range(tiles)):
            for c in range(chains):
                scaled_applied[c, j, pl.ds(r - TOP, DEEP), :] = hh[c] * value
    for c, sums in own_coefs(True):
        finish_coefs(True, c, sums)

    def step(k, carry):
        kick_hyper(k - 1, jnp.where(k == 1, 0.5, 1.0))
        drift_hyper()
        xs, ys = weights(1.0)
        mass = own_fresh(xs, ys)
        send(k + 1, predicted(xs, ys), mass)
        halo_advance(xs, ys)
        own_settle()
        pairs = list(own_coefs(False))
        halo_applied()
        for c, sums in pairs:
            finish_coefs(False, c, sums)
        return carry

    lax.fori_loop(1, STEPS, step, 0)

    for c in range(chains):
        for j in range(tiles):
            latent_out[c, :, pl.ds(j * LANES, LANES)] = state[c, j, own, :]
    kick_hyper(STEPS - 1, 1.0)
    drift_hyper()
    xs, ys = weights(0.5)
    for c in range(chains):
        x, y = xs[c][:1], ys[c][:1]
        for j in range(tiles):
            moved = field_u[c, j, own, :] - state[c, j, own, :] - 0.5 * scaled[c, j, own, :]
            moved = moved - x * applied[c, j, own, :] - y * intensity[c, j, own, :]
            momentum_out[c, :, pl.ds(j * LANES, LANES)] = moved * (1.0 / full(h[c])[:1])
    kick_hyper(STEPS, 0.5)

    out_row, out_col = sublane[:2, :2], lane[:2, :2]
    for high, low, ref in ((HYQ, HYE, hyper_out), (VEQ, VEE, velocity_out)):
        values = [[scal[base + c][:2, :2] for c in range(chains)] for base in (low, high)]
        pick = [jnp.where(out_col == 0, v[0], v[1]) for v in values]
        ref[...] = jnp.where(out_row == 0, pick[0], pick[1])

    def drain(k, carry):
        bulk(k).wait_send()
        return carry

    lax.fori_loop(0, STEPS + 1, drain, 0)


def hand_out(latent, momentum, hyper, velocity, latent_out, momentum_out, hyper_out, velocity_out, sems):
    copies = [
        pltpu.make_async_copy(latent, latent_out, sems.at[0]),
        pltpu.make_async_copy(momentum, momentum_out, sems.at[1]),
    ]
    for copy in copies:
        copy.start()
    hyper_out[...] = hyper[...]
    velocity_out[...] = velocity[...]
    for copy in copies:
        copy.wait()


def solution(mesh):
    nr, nc = mesh.shape["row"], mesh.shape["col"]
    devices = nr * nc

    def shards(latent, momentum, hyper_params, velocity, step_size, counts, kappa_field):
        chains, rows, cols = latent.shape
        tiles = cols // LANES
        deep = rows + 2 * TOP
        total = float(rows * nr * cols * nc)
        sizes = (nr, nc, chains, rows, tiles, total)
        anywhere = pl.BlockSpec(memory_space=pltpu.HBM)
        small = pl.BlockSpec(memory_space=pltpu.VMEM)
        arrays = 2 * chains + 2
        f32 = jnp.float32
        fold_one, fold_two = LANES // (SEG * chains), LANES // (SEG * (chains + 2))
        everywhere = pltpu.VMEM((chains, tiles + 1, deep, LANES), f32)
        inner = pltpu.VMEM((chains, tiles, rows, LANES), f32)
        strip_one = pltpu.VMEM((2, rows // fold_one, LANES), f32)
        strip_two = pltpu.VMEM((2, rows // fold_two, LANES), f32)
        corner = pltpu.VMEM((2, 2, HALO, LANES), f32)
        results = pl.pallas_call(
            functools.partial(kernel, sizes),
            out_shape=(
                jax.ShapeDtypeStruct(latent.shape, f32),
                jax.ShapeDtypeStruct(latent.shape, f32),
                jax.ShapeDtypeStruct(hyper_params.shape, f32),
                jax.ShapeDtypeStruct(velocity.shape, f32),
            ),
            in_specs=[anywhere] * 7,
            out_specs=(small,) * 4,
            scratch_shapes=[
                pltpu.VMEM((arrays, tiles + 1, deep, LANES), f32),
                everywhere,
                pltpu.VMEM((tiles + 1, deep, LANES), f32),
                everywhere,
                everywhere,
                everywhere,
                inner,
                inner,
                pltpu.VMEM((tiles, rows, LANES), jnp.int32),
                strip_one, strip_two, strip_one, strip_two, corner, corner,
                pltpu.VMEM((STEPS + 1, 1, LANES), f32),
                pltpu.VMEM((STEPS + 1, devices, 1, LANES), f32),
                pltpu.VMEM(((6 + COEFS) * chains + 1, 8, LANES), f32),
                pltpu.SMEM(hyper_params.shape, f32),
                pltpu.SMEM(velocity.shape, f32),
                pltpu.SMEM(step_size.shape, f32),
                pltpu.SemaphoreType.DMA((2 * tiles * (chains + 1) + 3,)),
                pltpu.SemaphoreType.DMA((18,)),
                pltpu.SemaphoreType.DMA((18,)),
                pltpu.SemaphoreType.DMA((STEPS + 1,)),
                pltpu.SemaphoreType.DMA((STEPS + 1,)),
                pltpu.SemaphoreType.REGULAR((len(signal_rounds(nr, nc)),)),
            ],
            compiler_params=pltpu.CompilerParams(
                collective_id=0, has_side_effects=True, vmem_limit_bytes=24 * 1024 * 1024
            ),
        )(*(pltpu.with_memory_space_constraint(x, pltpu.HBM) for x in (
            latent, momentum, counts, kappa_field, hyper_params, velocity, step_size
        )))
        return pl.pallas_call(
            hand_out,
            out_shape=[jax.ShapeDtypeStruct(x.shape, f32) for x in results],
            in_specs=[small] * 4,
            out_specs=[anywhere] * 2 + [small] * 2,
            scratch_shapes=[pltpu.SemaphoreType.DMA((2,))],
            compiler_params=pltpu.CompilerParams(vmem_limit_bytes=8 * 1024 * 1024),
        )(*results)

    placed = (
        P(None, "row", "col"),
        P(None, "row", "col"),
        P(),
        P(),
        P(),
        P("row", "col"),
        P("row", "col"),
    )
    return jax.shard_map(
        shards,
        mesh=mesh,
        in_specs=placed,
        out_specs=(P(None, "row", "col"), P(None, "row", "col"), P(), P()),
        check_vma=False,
    )
```

```python
import functools

import jax
import jax.numpy as jnp
from jax import lax
from jax.experimental import pallas as pl
from jax.experimental.pallas import tpu as pltpu
from jax.sharding import PartitionSpec as P

STEPS = 10
HALO = 16
EDGE = 8
NEEDED = STEPS + 1
PAD = 8
TOP = PAD + HALO
LANES = 128
SEG = 16
MESH = pl.DeviceIdType.MESH
COEFS = 6


def signal_rounds(nr, nc):
    rounds, reach = [], 1
    while reach < nr // 2 or reach < nc // 2:
        rs = (0, reach, -reach) if reach < nr // 2 else (0,)
        cs = (0, reach, -reach) if reach < nc // 2 else (0,)
        rounds.append([(r, c) for r in rs for c in cs if (r, c) != (0, 0)])
        reach *= 2
    return rounds


def kernel(
    sizes, latent, momentum, counts, kappa, hyper_in, velocity_in, step_in,
    latent_out, momentum_out, hyper_out, velocity_out,
    state, field_u, diagonal, applied, intensity, scaled, scaled_applied, fresh, raw_counts,
    pack_one, pack_two, take_one, take_two, corner_out, corner_in,
    payload, gathered, scal, hyper, velocity, step_size,
    load_sem, halo_send, halo_recv, sum_send, sum_recv, round_sem,
):
    nr, nc, chains, rows, tiles, total = sizes
    devices = nr * nc
    row, col = lax.axis_index("row"), lax.axis_index("col")
    me = row * nc + col
    kap, cnt = 2 * chains, 2 * chains + 1
    fold_one, fold_two = LANES // (SEG * chains), LANES // (SEG * (chains + 2))
    rows_one, rows_two = rows // fold_one, rows // fold_two
    own = pl.ds(TOP, rows)
    everything = range(tiles + 1)

    smalls = [(hyper_in, hyper), (velocity_in, velocity), (step_in, step_size)]
    vloads, loads = [], []
    for c in range(chains):
        for j in range(tiles):
            cols = pl.ds(j * LANES, LANES)
            vloads.append((latent.at[c, :, cols], state.at[c, j, own, :]))
            loads.append((momentum.at[c, :, cols], state.at[chains + c, j, own, :]))
    for j in range(tiles):
        cols = pl.ds(j * LANES, LANES)
        loads.append((kappa.at[:, cols], state.at[kap, j, own, :]))
        loads.append((counts.at[:, cols], raw_counts.at[j]))
    first_loads = len(vloads)
    loads = [
        pltpu.make_async_copy(s, d, load_sem.at[i]) for i, (s, d) in enumerate(vloads + loads + smalls)
    ]
    for copy in loads:
        copy.start()

    def at(dr, dc):
        return (lax.rem(row + (dr + nr), nr), lax.rem(col + (dc + nc), nc))

    near = [(r, c) for r in (0, 1, -1) for c in (0, 1, -1) if (r, c) != (0, 0)]
    barrier = pltpu.get_barrier_semaphore()
    for r, c in near:
        pl.semaphore_signal(barrier, inc=1, device_id=at(r, c), device_id_type=MESH)

    lane = lax.broadcasted_iota(jnp.int32, (8, LANES), 1)
    sublane = lax.broadcasted_iota(jnp.int32, (8, LANES), 0)
    lane_row = lax.broadcasted_iota(jnp.int32, (1, LANES), 1)
    seg = lane_row // SEG
    first, last = lane_row == 0, lane_row == LANES - 1

    def fold(x):
        return sum(x[8 * i : 8 * i + 8] for i in range(x.shape[0] // 8))

    def whole(x):
        return jnp.broadcast_to(jnp.sum(jnp.sum(x, axis=0, keepdims=True), axis=1, keepdims=True), (8, LANES))

    def pack(ref, arrays, depth, folds):
        heads = tails = None
        for s in range(folds):
            part = pl.ds(TOP + s * depth, depth)
            for i, a in enumerate(arrays):
                slot = s * len(arrays) + i
                head, tail = state[a, 0, part, :], state[a, tiles - 1, part, :]
                if slot:
                    head = pltpu.roll(head, slot * SEG, 1)
                tail = pltpu.roll(tail, (slot + 1) * SEG % LANES, 1) if (slot + 1) * SEG % LANES else tail
                heads = head if heads is None else jnp.where(seg == slot, head, heads)
                tails = tail if tails is None else jnp.where(seg == slot, tail, tails)
        ref[0] = heads
        ref[1] = tails

    def unpack(right, left, slot_right, slot_left):
        turn = (LANES - SEG * slot_right) % LANES
        right = pltpu.roll(right, turn, 1) if turn else right
        turn = (LANES - SEG - SEG * slot_left) % LANES
        left = pltpu.roll(left, turn, 1) if turn else left
        return jnp.where(seg == 0, right, jnp.where(seg == LANES // SEG - 1, left, 0.0))

    for copy in loads[:first_loads]:
        copy.wait()
    pack(pack_one, list(range(chains)), rows_one, fold_one)
    pl.semaphore_wait(barrier, len(near))

    remotes = []

    def remote(src, dst, where):
        copy = pltpu.make_async_remote_copy(
            src_ref=src, dst_ref=dst, send_sem=halo_send.at[len(remotes)], recv_sem=halo_recv.at[len(remotes)],
            device_id=where, device_id_type=MESH,
        )
        remotes.append(copy)
        copy.start()

    vs = pl.ds(0, chains)
    flat = pl.ds(0, tiles)

    def rowcopies(arrays, near_row, depth):
        remote(
            state.at[arrays, flat, pl.ds(TOP + near_row, depth), :],
            state.at[arrays, flat, pl.ds(TOP + rows + near_row, depth), :],
            at(-1, 0),
        )
        remote(
            state.at[arrays, flat, pl.ds(TOP + rows - near_row - depth, depth), :],
            state.at[arrays, flat, pl.ds(TOP - near_row - depth, depth), :],
            at(1, 0),
        )

    remote(pack_one.at[0], take_one.at[0], at(0, -1))
    remote(pack_one.at[1], take_one.at[1], at(0, 1))
    rowcopies(vs, 0, EDGE)
    stage_one = len(remotes)

    rounds = signal_rounds(nr, nc)

    def tell(i):
        for r, c in rounds[i]:
            pl.semaphore_signal(round_sem.at[i], inc=1, device_id=at(r, c), device_id_type=MESH)

    tell(0)

    for copy in loads[first_loads:]:
        copy.wait()
    rowcopies(pl.ds(chains, chains + 1), 0, NEEDED - 1)
    counted = jnp.zeros((8, LANES), jnp.float32)
    for j in range(tiles):
        value = raw_counts[j].astype(jnp.float32)
        state[cnt, j, own, :] = value
        counted += fold(value)
    for vert, start in ((1, TOP), (0, TOP + rows - HALO)):
        heads = tails = None
        for a in range(2 * chains + 2):
            head = state[a, 0, pl.ds(start, HALO), :]
            tail = pltpu.roll(state[a, tiles - 1, pl.ds(start, HALO), :], (a + 1) * SEG % LANES, 1)
            if a:
                head = pltpu.roll(head, a * SEG, 1)
            heads = head if heads is None else jnp.where(seg == a, head, heads)
            tails = tail if tails is None else jnp.where(seg == a, tail, tails)
        corner_out[0, vert] = heads
        corner_out[1, vert] = tails
    rowcopies(pl.ds(cnt, 1), 0, NEEDED - 1)
    for side, dc in ((0, -1), (1, 1)):
        for vert, dr in ((1, -1), (0, 1)):
            part = pl.ds(0 if vert else HALO - NEEDED, NEEDED)
            remote(corner_out.at[side, vert, part], corner_in.at[side, vert, part], at(dr, dc))
    rowcopies(vs, EDGE, NEEDED - EDGE)
    pack(pack_two, list(range(chains, 2 * chains + 2)), rows_two, fold_two)
    remote(pack_two.at[0], take_two.at[0], at(0, -1))
    remote(pack_two.at[1], take_two.at[1], at(0, 1))

    h = [step_size[c] for c in range(chains)]
    hh = [h[c] * h[c] for c in range(chains)]

    def full(value):
        return jnp.full((8, LANES), value, jnp.float32)

    TAU, EXO, HYQ, HYE, VEQ, VEE = (i * chains for i in range(6))
    CO = 6 * chains
    LOCAL = CO + COEFS * chains
    for c in range(chains):
        scal[HYQ + c] = full(hyper[1, c])
        scal[HYE + c] = full(hyper[0, c])
        scal[VEQ + c] = full(velocity[1, c])
        scal[VEE + c] = full(velocity[0, c])
        scal[TAU + c] = jnp.exp(full(hyper[1, c]))
        scal[EXO + c] = jnp.exp(full(hyper[0, c]))
    scal[LOCAL] = whole(counted)

    mass = []
    for c in range(chains):
        acc = None
        for j in range(tiles):
            value = jnp.exp(state[c, j, own, :])
            intensity[c, j, own, :] = value
            acc = fold(value) if acc is None else acc + fold(value)
        mass.append(whole(acc))
    for j in range(tiles):
        diagonal[j, own, :] = state[kap, j, own, :] + 4.0
        for c in range(chains):
            hc = hh[c] * state[cnt, j, own, :]
            scaled[c, j, own, :] = hc
            field_u[c, j, own, :] = state[c, j, own, :] + (h[c] * state[chains + c, j, own, :] + 0.5 * hc)

    def stencil(ref, c, r, deep, lane_tiles):
        rowset = pl.ds(r, deep)
        at_tile = [ref[c, j, rowset, :] for j in everything]
        n = tiles + 1
        used = sorted({(j + s) % n for j in lane_tiles for s in (-1, 0)})
        to_right = {j: pltpu.roll(at_tile[j], 1, 1) for j in used}
        used = sorted({(j + s) % n for j in lane_tiles for s in (1, 0)})
        to_left = {j: pltpu.roll(at_tile[j], LANES - 1, 1) for j in used}
        out = []
        for j in lane_tiles:
            beside = jnp.where(first, to_right[(j - 1) % n], to_right[j])
            beside += jnp.where(last, to_left[(j + 1) % n], to_left[j])
            beside += ref[c, j, pl.ds(r - 1, deep), :] + ref[c, j, pl.ds(r + 1, deep), :]
            out.append((j, at_tile[j], diagonal[j, rowset, :] * at_tile[j] - beside))
        return out

    DEEP = 64

    def own_blocks():
        return [TOP + i * DEEP for i in range(rows // DEEP)]

    def sides():
        out = [(TOP + i * DEEP, DEEP, [tiles]) for i in range(rows // DEEP)]
        return out + [(PAD, HALO, everything), (TOP + rows, HALO, everything)]

    def own_applied():
        quads = []
        for c in range(chains):
            acc = jnp.zeros((8, LANES), jnp.float32)
            for r in own_blocks():
                for j, v, av in stencil(state, c, r, DEEP, range(tiles)):
                    applied[c, j, pl.ds(r, DEEP), :] = av
                    acc += fold(v * av)
            quads.append(acc)
        return [whole(q) for q in quads]

    def halo_applied():
        for c in range(chains):
            for r, deep, lane_tiles in sides():
                for j, _, av in stencil(state, c, r, deep, lane_tiles):
                    applied[c, j, pl.ds(r, deep), :] = av

    others = sorted(range(1, devices), key=lambda d: -min(d, devices - d))

    def peer(d):
        other = lax.rem(me + d, devices)
        return (other // nc, lax.rem(other, nc))

    def send(k, quad, mass):
        out = scal[LOCAL][:1]
        for i, value in enumerate(quad + mass):
            out = jnp.where(seg == i, value[:1], out)
        payload[k] = out
        gathered[k, me] = out
        for d in others:
            pltpu.make_async_remote_copy(
                src_ref=payload.at[k], dst_ref=gathered.at[k, me],
                send_sem=sum_send.at[k], recv_sem=sum_recv.at[k],
                device_id=peer(d), device_id_type=MESH,
            ).start()

    def bulk(k):
        ref = gathered.at[k, pl.ds(0, devices - 1)]
        return pltpu.make_async_remote_copy(
            src_ref=ref, dst_ref=ref, send_sem=sum_send.at[k], recv_sem=sum_recv.at[k],
            device_id=peer(1), device_id_type=MESH,
        )

    def collect(k):
        bulk(k).wait_recv()
        summed = jnp.broadcast_to(jnp.sum(gathered[k], axis=0), (8, LANES))
        values = [
            jnp.broadcast_to(jnp.sum(jnp.where(lane == i * SEG, summed, 0.0), axis=1, keepdims=True), (8, LANES))
            for i in range(2 * chains + 1)
        ]
        return values[:chains], values[chains : 2 * chains], values[2 * chains]

    def kick_hyper(k, part):
        quad, mass, number = collect(k)
        for c in range(chains):
            aq = (0.5 / total) * (scal[TAU + c] * quad[c]) - 0.5
            ae = (scal[EXO + c] * mass[c] - number) * (1.0 / total)
            scal[VEQ + c] = scal[VEQ + c] - (part * h[c]) * aq
            scal[VEE + c] = scal[VEE + c] - (part * h[c]) * ae

    def drift_hyper():
        for c in range(chains):
            q = scal[HYQ + c] + h[c] * scal[VEQ + c]
            e = scal[HYE + c] + h[c] * scal[VEE + c]
            scal[HYQ + c] = q
            scal[HYE + c] = e
            scal[TAU + c] = jnp.exp(q)
            scal[EXO + c] = jnp.exp(e)

    def weights(part):
        xs = [(part * hh[c]) * scal[TAU + c] for c in range(chains)]
        ys = [(part * hh[c]) * scal[EXO + c] for c in range(chains)]
        return xs, ys

    def own_fresh(xs, ys):
        out = []
        for c in range(chains):
            x, y = xs[c][:1], ys[c][:1]
            acc = jnp.zeros((8, LANES), jnp.float32)
            for j in range(tiles):
                v = field_u[c, j, own, :] - x * applied[c, j, own, :] - y * intensity[c, j, own, :]
                value = jnp.exp(v)
                fresh[c, j] = v
                intensity[c, j, own, :] = value
                acc += fold(value)
            out.append(acc)
        return [whole(acc) for acc in out]

    def own_settle():
        for c in range(chains):
            for j in range(tiles):
                v = fresh[c, j]
                field_u[c, j, own, :] = (v + v) - state[c, j, own, :] + scaled[c, j, own, :]
                state[c, j, own, :] = v

    def halo_advance(xs, ys):
        for c in range(chains):
            x, y = xs[c][:1], ys[c][:1]
            for r, deep, lane_tiles in sides():
                rowset = pl.ds(r, deep)
                for j in lane_tiles:
                    v = field_u[c, j, rowset, :] - x * applied[c, j, rowset, :] - y * intensity[c, j, rowset, :]
                    field_u[c, j, rowset, :] = (v + v) - state[c, j, rowset, :] + scaled[c, j, rowset, :]
                    intensity[c, j, rowset, :] = jnp.exp(v)
                    state[c, j, rowset, :] = v

    def own_coefs(direct):
        for c in range(chains):
            sums = [jnp.zeros((8, LANES), jnp.float32)] * COEFS
            if not direct:
                for r in own_blocks():
                    rowset = pl.ds(r, DEEP)
                    for j, v, av in stencil(state, c, r, DEEP, range(tiles)):
                        au = (av + av) - applied[c, j, rowset, :] + scaled_applied[c, j, pl.ds(r - TOP, DEEP), :]
                        applied[c, j, rowset, :] = av
                        sums[0] += fold(field_u[c, j, rowset, :] * au)
                        sums[1] += fold(av * au)
                        sums[2] += fold(intensity[c, j, rowset, :] * au)
            yield c, sums

    def finish_coefs(direct, c, sums):
        for r in own_blocks():
            rowset = pl.ds(r, DEEP)
            if direct:
                for j, u, au in stencil(field_u, c, r, DEEP, range(tiles)):
                    sums[0] += fold(u * au)
                    sums[1] += fold(applied[c, j, rowset, :] * au)
                    sums[2] += fold(intensity[c, j, rowset, :] * au)
            for j, a, aa in stencil(applied, c, r, DEEP, range(tiles)):
                sums[3] += fold(a * aa)
                sums[4] += fold(intensity[c, j, rowset, :] * aa)
            for j, e, ae in stencil(intensity, c, r, DEEP, range(tiles)):
                sums[5] += fold(e * ae)
        for i in range(COEFS):
            scal[CO + COEFS * c + i] = whole(sums[i])

    def predicted(xs, ys):
        out = []
        for c in range(chains):
            k0, k1, k2, k3, k4, k5 = [scal[CO + COEFS * c + i] for i in range(COEFS)]
            x, y = xs[c], ys[c]
            out.append(k0 - 2.0 * (x * k1 + y * k2) + (x * (x * k3 + 2.0 * (y * k4)) + y * (y * k5)))
        return out

    for i in range(len(rounds)):
        pl.semaphore_wait(round_sem.at[i], len(rounds[i]))
        if i + 1 < len(rounds):
            tell(i + 1)
        if i == 0:
            for copy in remotes[:stage_one]:
                copy.wait_recv()
            for c in range(chains):
                for s in range(fold_one):
                    slot = s * chains + c
                    state[c, tiles, pl.ds(TOP + s * rows_one, rows_one), :] = unpack(
                        take_one[0], take_one[1], slot, slot
                    )
            quad = own_applied()
    send(0, quad, mass)

    xs, ys = weights(0.5)
    mass = own_fresh(xs, ys)

    for copy in remotes[stage_one:]:
        copy.wait_recv()
    for copy in remotes:
        copy.wait_send()

    for s in range(fold_two):
        for i in range(chains + 2):
            slot = s * (chains + 2) + i
            state[chains + i, tiles, pl.ds(TOP + s * rows_two, rows_two), :] = unpack(
                take_two[0], take_two[1], slot, slot
            )
    for vert, r in ((0, PAD), (1, TOP + rows)):
        for a in range(2 * chains + 2):
            state[a, tiles, pl.ds(r, HALO), :] = unpack(corner_in[0, vert], corner_in[1, vert], a, a)
    for r, deep, lane_tiles in sides():
        rowset = pl.ds(r, deep)
        for j in lane_tiles:
            diagonal[j, rowset, :] = state[kap, j, rowset, :] + 4.0
            for c in range(chains):
                hc = hh[c] * state[cnt, j, rowset, :]
                scaled[c, j, rowset, :] = hc
                v = state[c, j, rowset, :]
                intensity[c, j, rowset, :] = jnp.exp(v)
                field_u[c, j, rowset, :] = v + (h[c] * state[chains + c, j, rowset, :] + 0.5 * hc)
    halo_applied()
    halo_advance(xs, ys)
    own_settle()
    send(1, own_applied(), mass)
    halo_applied()
    for r in own_blocks():
        for j, _, value in stencil(state, cnt, r, DEEP, range(tiles)):
            for c in range(chains):
                scaled_applied[c, j, pl.ds(r - TOP, DEEP), :] = hh[c] * value
    for c, sums in own_coefs(True):
        finish_coefs(True, c, sums)

    def step(k, carry):
        kick_hyper(k - 1, jnp.where(k == 1, 0.5, 1.0))
        drift_hyper()
        xs, ys = weights(1.0)
        mass = own_fresh(xs, ys)
        send(k + 1, predicted(xs, ys), mass)
        halo_advance(xs, ys)
        own_settle()
        pairs = list(own_coefs(False))
        halo_applied()
        for c, sums in pairs:
            finish_coefs(False, c, sums)
        return carry

    lax.fori_loop(1, STEPS, step, 0)

    for c in range(chains):
        for j in range(tiles):
            latent_out[c, :, pl.ds(j * LANES, LANES)] = state[c, j, own, :]
    kick_hyper(STEPS - 1, 1.0)
    drift_hyper()
    xs, ys = weights(0.5)
    for c in range(chains):
        x, y = xs[c][:1], ys[c][:1]
        for j in range(tiles):
            moved = field_u[c, j, own, :] - state[c, j, own, :] - 0.5 * scaled[c, j, own, :]
            moved = moved - x * applied[c, j, own, :] - y * intensity[c, j, own, :]
            momentum_out[c, :, pl.ds(j * LANES, LANES)] = moved * (1.0 / full(h[c])[:1])
    kick_hyper(STEPS, 0.5)

    out_row, out_col = sublane[:2, :2], lane[:2, :2]
    for high, low, ref in ((HYQ, HYE, hyper_out), (VEQ, VEE, velocity_out)):
        values = [[scal[base + c][:2, :2] for c in range(chains)] for base in (low, high)]
        pick = [jnp.where(out_col == 0, v[0], v[1]) for v in values]
        ref[...] = jnp.where(out_row == 0, pick[0], pick[1])

    def drain(k, carry):
        bulk(k).wait_send()
        return carry

    lax.fori_loop(0, STEPS + 1, drain, 0)


def hand_out(*refs):
    count = (len(refs) - 1) // 2
    sems = refs[-1]
    copies = [pltpu.make_async_copy(refs[i], refs[count + i], sems.at[i]) for i in range(count)]
    for copy in copies:
        copy.start()
    for copy in copies:
        copy.wait()


def solution(mesh):
    nr, nc = mesh.shape["row"], mesh.shape["col"]
    devices = nr * nc

    def shards(latent, momentum, hyper_params, velocity, step_size, counts, kappa_field):
        chains, rows, cols = latent.shape
        tiles = cols // LANES
        deep = rows + 2 * TOP
        total = float(rows * nr * cols * nc)
        sizes = (nr, nc, chains, rows, tiles, total)
        anywhere = pl.BlockSpec(memory_space=pltpu.HBM)
        small = pl.BlockSpec(memory_space=pltpu.VMEM)
        arrays = 2 * chains + 2
        f32 = jnp.float32
        fold_one, fold_two = LANES // (SEG * chains), LANES // (SEG * (chains + 2))
        everywhere = pltpu.VMEM((chains, tiles + 1, deep, LANES), f32)
        inner = pltpu.VMEM((chains, tiles, rows, LANES), f32)
        strip_one = pltpu.VMEM((2, rows // fold_one, LANES), f32)
        strip_two = pltpu.VMEM((2, rows // fold_two, LANES), f32)
        corner = pltpu.VMEM((2, 2, HALO, LANES), f32)
        results = pl.pallas_call(
            functools.partial(kernel, sizes),
            out_shape=(
                jax.ShapeDtypeStruct(latent.shape, f32),
                jax.ShapeDtypeStruct(latent.shape, f32),
                jax.ShapeDtypeStruct(hyper_params.shape, f32),
                jax.ShapeDtypeStruct(velocity.shape, f32),
            ),
            in_specs=[anywhere] * 7,
            out_specs=(small,) * 4,
            scratch_shapes=[
                pltpu.VMEM((arrays, tiles + 1, deep, LANES), f32),
                everywhere,
                pltpu.VMEM((tiles + 1, deep, LANES), f32),
                everywhere,
                everywhere,
                everywhere,
                inner,
                inner,
                pltpu.VMEM((tiles, rows, LANES), jnp.int32),
                strip_one, strip_two, strip_one, strip_two, corner, corner,
                pltpu.VMEM((STEPS + 1, 1, LANES), f32),
                pltpu.VMEM((STEPS + 1, devices, 1, LANES), f32),
                pltpu.VMEM(((6 + COEFS) * chains + 1, 8, LANES), f32),
                pltpu.SMEM(hyper_params.shape, f32),
                pltpu.SMEM(velocity.shape, f32),
                pltpu.SMEM(step_size.shape, f32),
                pltpu.SemaphoreType.DMA((2 * tiles * (chains + 1) + 3,)),
                pltpu.SemaphoreType.DMA((16,)),
                pltpu.SemaphoreType.DMA((16,)),
                pltpu.SemaphoreType.DMA((STEPS + 1,)),
                pltpu.SemaphoreType.DMA((STEPS + 1,)),
                pltpu.SemaphoreType.REGULAR((len(signal_rounds(nr, nc)),)),
            ],
            compiler_params=pltpu.CompilerParams(
                collective_id=0, has_side_effects=True, vmem_limit_bytes=24 * 1024 * 1024
            ),
        )(*(pltpu.with_memory_space_constraint(x, pltpu.HBM) for x in (
            latent, momentum, counts, kappa_field, hyper_params, velocity, step_size
        )))
        return pl.pallas_call(
            hand_out,
            out_shape=[jax.ShapeDtypeStruct(x.shape, f32) for x in results],
            in_specs=[small] * 4,
            out_specs=[pl.BlockSpec(memory_space=pl.ANY)] * 4,
            scratch_shapes=[pltpu.SemaphoreType.DMA((4,))],
            compiler_params=pltpu.CompilerParams(vmem_limit_bytes=8 * 1024 * 1024),
        )(*results)

    placed = (
        P(None, "row", "col"),
        P(None, "row", "col"),
        P(),
        P(),
        P(),
        P("row", "col"),
        P("row", "col"),
    )
    return jax.shard_map(
        shards,
        mesh=mesh,
        in_specs=placed,
        out_specs=(P(None, "row", "col"), P(None, "row", "col"), P(), P()),
        check_vma=False,
    )
```

```python
import functools

import jax
import jax.numpy as jnp
from jax import lax
from jax.experimental import pallas as pl
from jax.experimental.pallas import tpu as pltpu
from jax.sharding import PartitionSpec as P

STEPS = 10
HALO = 16
EDGE = 8
NEEDED = STEPS + 1
PAD = 8
TOP = PAD + HALO
LANES = 128
SEG = 16
MESH, LOGICAL = pl.DeviceIdType.MESH, pl.DeviceIdType.LOGICAL
COEFS = 6


def signal_rounds(nr):
    rounds, reach = [], 1
    while reach < nr // 2:
        rounds.append(reach)
        reach *= 2
    return rounds


def kernel(
    sizes, latent, momentum, counts, kappa, hyper_in, velocity_in, step_in,
    latent_out, momentum_out, hyper_out, velocity_out,
    state, field_u, diagonal, applied, intensity, scaled, scaled_applied, fresh, raw_counts,
    padded, half, pack_one, pack_two, take_one, take_two, corner_out, corner_in,
    payload, gathered, scal, hyper, velocity, step_size,
    load_sem, halo_send, halo_recv, sum_send, sum_recv, round_sem,
):
    nr, nc, chains, rows, tiles, total = sizes
    devices = nr * nc
    row, col = lax.axis_index("row"), lax.axis_index("col")
    me = row * nc + col
    kap, cnt = 2 * chains, 2 * chains + 1
    fold_one, fold_two = LANES // (SEG * chains), LANES // (SEG * (chains + 2))
    rows_one, rows_two = rows // fold_one, rows // fold_two
    own = pl.ds(TOP, rows)
    everything = range(tiles + 1)

    smalls = [(hyper_in, hyper), (velocity_in, velocity), (step_in, step_size)]
    vloads, loads = [], []
    for c in range(chains):
        for j in range(tiles):
            cols = pl.ds(j * LANES, LANES)
            vloads.append((latent.at[c, :, cols], state.at[c, j, own, :]))
            loads.append((momentum.at[c, :, cols], state.at[chains + c, j, own, :]))
    for j in range(tiles):
        cols = pl.ds(j * LANES, LANES)
        loads.append((kappa.at[:, cols], state.at[kap, j, own, :]))
        loads.append((counts.at[:, cols], raw_counts.at[j]))
    first_loads = len(vloads)
    loads = [
        pltpu.make_async_copy(s, d, load_sem.at[i]) for i, (s, d) in enumerate(vloads + loads + smalls)
    ]
    for copy in loads:
        copy.start()

    def wrap(d):
        other = me + d % devices
        return jnp.where(other < devices, other, other - devices)

    def at(dr, dc):
        return (lax.rem(row + (dr + nr), nr), lax.rem(col + (dc + nc), nc))

    barrier = pltpu.get_barrier_semaphore()
    near = [lax.rem(row + r, nr) * nc + c for r in (1, nr - 1) for c in range(nc)]
    near += [row * nc + jnp.where(col + c < nc, col + c, col + c - nc) for c in range(1, nc)]
    for other in near:
        pl.semaphore_signal(barrier, inc=1, device_id=other, device_id_type=LOGICAL)
    others = [wrap(d) for d in sorted(range(1, devices), key=lambda d: -min(d, devices - d))]

    lane = lax.broadcasted_iota(jnp.int32, (8, LANES), 1)
    sublane = lax.broadcasted_iota(jnp.int32, (8, LANES), 0)
    lane_row = lax.broadcasted_iota(jnp.int32, (1, LANES), 1)
    seg = lane_row // SEG
    first, last = lane_row == 0, lane_row == LANES - 1

    def fold(x):
        return sum(x[8 * i : 8 * i + 8] for i in range(x.shape[0] // 8))

    def whole(x):
        return jnp.broadcast_to(jnp.sum(jnp.sum(x, axis=0, keepdims=True), axis=1, keepdims=True), (8, LANES))

    def pack(ref, arrays, depth, folds):
        heads = tails = None
        for s in range(folds):
            part = pl.ds(TOP + s * depth, depth)
            for i, a in enumerate(arrays):
                slot = s * len(arrays) + i
                head, tail = state[a, 0, part, :], state[a, tiles - 1, part, :]
                if slot:
                    head = pltpu.roll(head, slot * SEG, 1)
                tail = pltpu.roll(tail, (slot + 1) * SEG % LANES, 1) if (slot + 1) * SEG % LANES else tail
                heads = head if heads is None else jnp.where(seg == slot, head, heads)
                tails = tail if tails is None else jnp.where(seg == slot, tail, tails)
        ref[0] = heads
        ref[1] = tails

    def unpack(right, left, slot_right, slot_left):
        turn = (LANES - SEG * slot_right) % LANES
        right = pltpu.roll(right, turn, 1) if turn else right
        turn = (LANES - SEG - SEG * slot_left) % LANES
        left = pltpu.roll(left, turn, 1) if turn else left
        return jnp.where(seg == 0, right, jnp.where(seg == LANES // SEG - 1, left, 0.0))

    for copy in loads[:first_loads]:
        copy.wait()
    pack(pack_one, list(range(chains)), rows_one, fold_one)
    pl.semaphore_wait(barrier, len(near))

    remotes = []

    def remote(src, dst, where):
        copy = pltpu.make_async_remote_copy(
            src_ref=src, dst_ref=dst, send_sem=halo_send.at[len(remotes)], recv_sem=halo_recv.at[len(remotes)],
            device_id=where, device_id_type=MESH,
        )
        remotes.append(copy)
        copy.start()

    vs = pl.ds(0, chains)
    flat = pl.ds(0, tiles)

    def rowcopies(arrays, near_row, depth):
        remote(
            state.at[arrays, flat, pl.ds(TOP + near_row, depth), :],
            state.at[arrays, flat, pl.ds(TOP + rows + near_row, depth), :],
            at(-1, 0),
        )
        remote(
            state.at[arrays, flat, pl.ds(TOP + rows - near_row - depth, depth), :],
            state.at[arrays, flat, pl.ds(TOP - near_row - depth, depth), :],
            at(1, 0),
        )

    remote(pack_one.at[0], take_one.at[0], at(0, -1))
    remote(pack_one.at[1], take_one.at[1], at(0, 1))
    rowcopies(vs, 0, EDGE)
    stage_one = len(remotes)

    rounds = signal_rounds(nr)

    def tell(i):
        for r in (rounds[i], -rounds[i]):
            pl.semaphore_signal(round_sem.at[i], inc=1, device_id=at(r, 0), device_id_type=MESH)

    tell(0)

    for copy in loads[first_loads:]:
        copy.wait()
    rowcopies(pl.ds(chains, chains + 1), 0, NEEDED - 1)
    counted = jnp.zeros((8, LANES), jnp.float32)
    for j in range(tiles):
        value = raw_counts[j].astype(jnp.float32)
        state[cnt, j, own, :] = value
        counted += fold(value)
    for vert, start in ((1, TOP), (0, TOP + rows - HALO)):
        heads = tails = None
        for a in range(2 * chains + 2):
            head = state[a, 0, pl.ds(start, HALO), :]
            tail = pltpu.roll(state[a, tiles - 1, pl.ds(start, HALO), :], (a + 1) * SEG % LANES, 1)
            if a:
                head = pltpu.roll(head, a * SEG, 1)
            heads = head if heads is None else jnp.where(seg == a, head, heads)
            tails = tail if tails is None else jnp.where(seg == a, tail, tails)
        corner_out[0, vert] = heads
        corner_out[1, vert] = tails
    rowcopies(pl.ds(cnt, 1), 0, NEEDED - 1)
    for side, dc in ((0, -1), (1, 1)):
        for vert, dr in ((1, -1), (0, 1)):
            part = pl.ds(0 if vert else HALO - NEEDED, NEEDED)
            remote(corner_out.at[side, vert, part], corner_in.at[side, vert, part], at(dr, dc))
    rowcopies(vs, EDGE, NEEDED - EDGE)
    pack(pack_two, list(range(chains, 2 * chains + 2)), rows_two, fold_two)
    remote(pack_two.at[0], take_two.at[0], at(0, -1))
    remote(pack_two.at[1], take_two.at[1], at(0, 1))

    h = [step_size[c] for c in range(chains)]
    hh = [h[c] * h[c] for c in range(chains)]

    def full(value):
        return jnp.full((8, LANES), value, jnp.float32)

    TAU, EXO, HYQ, HYE, VEQ, VEE = (i * chains for i in range(6))
    CO = 6 * chains
    LOCAL = CO + COEFS * chains
    for c in range(chains):
        scal[HYQ + c] = full(hyper[1, c])
        scal[HYE + c] = full(hyper[0, c])
        scal[VEQ + c] = full(velocity[1, c])
        scal[VEE + c] = full(velocity[0, c])
        scal[TAU + c] = jnp.exp(full(hyper[1, c]))
        scal[EXO + c] = jnp.exp(full(hyper[0, c]))
    scal[LOCAL] = whole(counted)

    mass = []
    for c in range(chains):
        acc = None
        for j in range(tiles):
            value = jnp.exp(state[c, j, own, :])
            intensity[c, j, own, :] = value
            acc = fold(value) if acc is None else acc + fold(value)
        mass.append(whole(acc))
    for j in range(tiles):
        diag = state[kap, j, own, :] + 4.0
        diagonal[j, own, :] = diag
        half[j] = 0.5 * diag
        for c in range(chains):
            hc = hh[c] * state[cnt, j, own, :]
            scaled[c, j, own, :] = hc
            field_u[c, j, own, :] = state[c, j, own, :] + (h[c] * state[chains + c, j, own, :] + 0.5 * hc)

    def stencil(ref, c, r, deep, lane_tiles):
        rowset = pl.ds(r, deep)
        at_tile = [ref[c, j, rowset, :] for j in everything]
        n = tiles + 1
        used = sorted({(j + s) % n for j in lane_tiles for s in (-1, 0)})
        to_right = {j: pltpu.roll(at_tile[j], 1, 1) for j in used}
        used = sorted({(j + s) % n for j in lane_tiles for s in (1, 0)})
        to_left = {j: pltpu.roll(at_tile[j], LANES - 1, 1) for j in used}
        out = []
        for j in lane_tiles:
            beside = jnp.where(first, to_right[(j - 1) % n], to_right[j])
            beside += jnp.where(last, to_left[(j + 1) % n], to_left[j])
            beside += ref[c, j, pl.ds(r - 1, deep), :] + ref[c, j, pl.ds(r + 1, deep), :]
            out.append((j, at_tile[j], diagonal[j, rowset, :] * at_tile[j] - beside))
        return out

    def half_stencil(ref, c, r, deep):
        rowset = pl.ds(r, deep)
        at_tile = [ref[c, j, rowset, :] for j in everything]
        to_left = [pltpu.roll(x, LANES - 1, 1) for x in at_tile]
        out = []
        for j in range(tiles):
            beside = jnp.where(last, to_left[j + 1], to_left[j]) + ref[c, j, pl.ds(r + 1, deep), :]
            out.append((j, at_tile[j], half[j, pl.ds(r - TOP, deep), :] * at_tile[j] - beside))
        return out

    DEEP = 64

    def own_blocks():
        return [TOP + i * DEEP for i in range(rows // DEEP)]

    def sides():
        out = [(TOP + i * DEEP, DEEP, [tiles]) for i in range(rows // DEEP)]
        return out + [(PAD, HALO, everything), (TOP + rows, HALO, everything)]

    def own_applied(ref):
        quads = []
        for c in range(chains):
            acc = jnp.zeros((8, LANES), jnp.float32)
            for r in own_blocks():
                for j, v, av in stencil(ref, c, r, DEEP, range(tiles)):
                    applied[c, j, pl.ds(r, DEEP), :] = av
                    acc += fold(v * av)
            quads.append(acc)
        return quads

    def halo_applied():
        for c in range(chains):
            for r, deep, lane_tiles in sides():
                for j, _, av in stencil(state, c, r, deep, lane_tiles):
                    applied[c, j, pl.ds(r, deep), :] = av

    def send(k, quad, mass):
        out = scal[LOCAL][:1]
        for i, value in enumerate(quad + mass):
            out = jnp.where(seg == i, value[:1], out)
        payload[k] = out
        gathered[k, me] = out
        for other in others:
            pltpu.make_async_remote_copy(
                src_ref=payload.at[k], dst_ref=gathered.at[k, me],
                send_sem=sum_send.at[k], recv_sem=sum_recv.at[k],
                device_id=other, device_id_type=LOGICAL,
            ).start()

    def bulk(k):
        ref = gathered.at[k, pl.ds(0, devices - 1)]
        return pltpu.make_async_remote_copy(
            src_ref=ref, dst_ref=ref, send_sem=sum_send.at[k], recv_sem=sum_recv.at[k],
            device_id=others[0], device_id_type=LOGICAL,
        )

    def collect(k):
        bulk(k).wait_recv()
        summed = jnp.broadcast_to(jnp.sum(gathered[k], axis=0), (8, LANES))
        values = [
            jnp.broadcast_to(jnp.sum(jnp.where(lane == i * SEG, summed, 0.0), axis=1, keepdims=True), (8, LANES))
            for i in range(2 * chains + 1)
        ]
        return values[:chains], values[chains : 2 * chains], values[2 * chains]

    def kick_hyper(k, part):
        quad, mass, number = collect(k)
        for c in range(chains):
            aq = (0.5 / total) * (scal[TAU + c] * quad[c]) - 0.5
            ae = (scal[EXO + c] * mass[c] - number) * (1.0 / total)
            scal[VEQ + c] = scal[VEQ + c] - (part * h[c]) * aq
            scal[VEE + c] = scal[VEE + c] - (part * h[c]) * ae

    def drift_hyper():
        for c in range(chains):
            q = scal[HYQ + c] + h[c] * scal[VEQ + c]
            e = scal[HYE + c] + h[c] * scal[VEE + c]
            scal[HYQ + c] = q
            scal[HYE + c] = e
            scal[TAU + c] = jnp.exp(q)
            scal[EXO + c] = jnp.exp(e)

    def weights(part):
        xs = [(part * hh[c]) * scal[TAU + c] for c in range(chains)]
        ys = [(part * hh[c]) * scal[EXO + c] for c in range(chains)]
        return xs, ys

    def own_fresh(xs, ys):
        out = []
        for c in range(chains):
            x, y = xs[c][:1], ys[c][:1]
            acc = jnp.zeros((8, LANES), jnp.float32)
            for j in range(tiles):
                v = field_u[c, j, own, :] - x * applied[c, j, own, :] - y * intensity[c, j, own, :]
                value = jnp.exp(v)
                fresh[c, j] = v
                intensity[c, j, own, :] = value
                acc += fold(value)
            out.append(acc)
        return [whole(acc) for acc in out]

    def own_settle():
        for c in range(chains):
            for j in range(tiles):
                v = fresh[c, j]
                field_u[c, j, own, :] = (v + v) - state[c, j, own, :] + scaled[c, j, own, :]
                state[c, j, own, :] = v

    def halo_advance(xs, ys):
        for c in range(chains):
            x, y = xs[c][:1], ys[c][:1]
            for r, deep, lane_tiles in sides():
                rowset = pl.ds(r, deep)
                for j in lane_tiles:
                    v = field_u[c, j, rowset, :] - x * applied[c, j, rowset, :] - y * intensity[c, j, rowset, :]
                    field_u[c, j, rowset, :] = (v + v) - state[c, j, rowset, :] + scaled[c, j, rowset, :]
                    intensity[c, j, rowset, :] = jnp.exp(v)
                    state[c, j, rowset, :] = v

    def own_coefs(direct):
        for c in range(chains):
            sums = [jnp.zeros((8, LANES), jnp.float32)] * COEFS
            if not direct:
                for r in own_blocks():
                    rowset = pl.ds(r, DEEP)
                    for j, v, av in stencil(state, c, r, DEEP, range(tiles)):
                        au = (av + av) - applied[c, j, rowset, :] + scaled_applied[c, j, pl.ds(r - TOP, DEEP), :]
                        applied[c, j, rowset, :] = av
                        sums[0] += fold(field_u[c, j, rowset, :] * au)
                        sums[1] += fold(av * au)
                        sums[2] += fold(intensity[c, j, rowset, :] * au)
            yield c, sums

    def finish_coefs(direct, c, sums):
        for r in own_blocks():
            rowset = pl.ds(r, DEEP)
            if direct:
                for j, u, au in stencil(field_u, c, r, DEEP, range(tiles)):
                    sums[0] += fold(u * au)
                    sums[1] += fold(applied[c, j, rowset, :] * au)
                    sums[2] += fold(intensity[c, j, rowset, :] * au)
            for (j, a, ta), (_, e, te) in zip(half_stencil(applied, c, r, DEEP), half_stencil(intensity, c, r, DEEP)):
                sums[3] += fold(a * ta)
                sums[4] += fold(e * ta + a * te)
                sums[5] += fold(e * te)
        for i in range(COEFS):
            total_i = whole(sums[i])
            scal[CO + COEFS * c + i] = total_i + total_i if i in (3, 5) else total_i

    def predicted(xs, ys):
        out = []
        for c in range(chains):
            k0, k1, k2, k3, k4, k5 = [scal[CO + COEFS * c + i] for i in range(COEFS)]
            x, y = xs[c], ys[c]
            out.append(k0 - 2.0 * (x * k1 + y * k2) + (x * (x * k3 + 2.0 * (y * k4)) + y * (y * k5)))
        return out

    for c in range(chains):
        for r in (TOP - 8, TOP + rows):
            for j in range(tiles):
                padded[c, j, pl.ds(r, 8), :] = jnp.zeros((8, LANES), jnp.float32)
        padded[c, tiles, own, :] = jnp.zeros((rows, LANES), jnp.float32)
        for j in range(tiles):
            padded[c, j, own, :] = state[c, j, own, :]
    quad = own_applied(padded)
    place = lane_row % SEG

    for i in range(len(rounds)):
        pl.semaphore_wait(round_sem.at[i], 2)
        if i + 1 < len(rounds):
            tell(i + 1)
    for copy in remotes[:stage_one]:
        copy.wait_recv()
    across = jnp.where(place == SEG - 1, pack_one[1] * pltpu.roll(take_one[0], SEG - 1, 1), 0.0)
    across += jnp.where(place == 0, pack_one[0] * pltpu.roll(take_one[1], LANES - SEG + 1, 1), 0.0)
    across = fold(across)
    for c in range(chains):
        along = sum(
            state[c, j, pl.ds(TOP, 1), :] * state[c, j, pl.ds(TOP - 1, 1), :]
            + state[c, j, pl.ds(TOP + rows - 1, 1), :] * state[c, j, pl.ds(TOP + rows, 1), :]
            for j in range(tiles)
        )
        quad[c] = whole(quad[c] - jnp.where(seg % chains == c, across, 0.0) - jnp.where(sublane == 0, along, 0.0))
    send(0, quad, mass)

    for c in range(chains):
        for s in range(fold_one):
            slot = s * chains + c
            part = pl.ds(TOP + s * rows_one, rows_one)
            side = unpack(take_one[0], take_one[1], slot, slot)
            state[c, tiles, part, :] = side
            applied[c, 0, part, :] = applied[c, 0, part, :] - jnp.where(first, pltpu.roll(side, 1, 1), 0.0)
            applied[c, tiles - 1, part, :] = applied[c, tiles - 1, part, :] - jnp.where(
                last, pltpu.roll(side, LANES - 1, 1), 0.0
            )
        for j in range(tiles):
            for here, there in ((TOP, TOP - 1), (TOP + rows - 1, TOP + rows)):
                here, there = pl.ds(here, 1), pl.ds(there, 1)
                applied[c, j, here, :] = applied[c, j, here, :] - state[c, j, there, :]

    xs, ys = weights(0.5)
    mass = own_fresh(xs, ys)

    for copy in remotes[stage_one:]:
        copy.wait_recv()
    for copy in remotes:
        copy.wait_send()

    for s in range(fold_two):
        for i in range(chains + 2):
            slot = s * (chains + 2) + i
            state[chains + i, tiles, pl.ds(TOP + s * rows_two, rows_two), :] = unpack(
                take_two[0], take_two[1], slot, slot
            )
    for vert, r in ((0, PAD), (1, TOP + rows)):
        for a in range(2 * chains + 2):
            state[a, tiles, pl.ds(r, HALO), :] = unpack(corner_in[0, vert], corner_in[1, vert], a, a)
    for r, deep, lane_tiles in sides():
        rowset = pl.ds(r, deep)
        for j in lane_tiles:
            diagonal[j, rowset, :] = state[kap, j, rowset, :] + 4.0
            for c in range(chains):
                hc = hh[c] * state[cnt, j, rowset, :]
                scaled[c, j, rowset, :] = hc
                v = state[c, j, rowset, :]
                intensity[c, j, rowset, :] = jnp.exp(v)
                field_u[c, j, rowset, :] = v + (h[c] * state[chains + c, j, rowset, :] + 0.5 * hc)
    halo_applied()
    halo_advance(xs, ys)
    own_settle()
    send(1, [whole(q) for q in own_applied(state)], mass)
    halo_applied()
    for r in own_blocks():
        for j, _, value in stencil(state, cnt, r, DEEP, range(tiles)):
            for c in range(chains):
                scaled_applied[c, j, pl.ds(r - TOP, DEEP), :] = hh[c] * value
    for c, sums in own_coefs(True):
        finish_coefs(True, c, sums)

    def step(k, carry):
        kick_hyper(k - 1, jnp.where(k == 1, 0.5, 1.0))
        drift_hyper()
        xs, ys = weights(1.0)
        mass = own_fresh(xs, ys)
        send(k + 1, predicted(xs, ys), mass)
        halo_advance(xs, ys)
        own_settle()
        pairs = list(own_coefs(False))
        halo_applied()
        for c, sums in pairs:
            finish_coefs(False, c, sums)
        return carry

    lax.fori_loop(1, STEPS, step, 0)

    for c in range(chains):
        for j in range(tiles):
            latent_out[c, :, pl.ds(j * LANES, LANES)] = state[c, j, own, :]
    kick_hyper(STEPS - 1, 1.0)
    drift_hyper()
    xs, ys = weights(0.5)
    for c in range(chains):
        x, y = xs[c][:1], ys[c][:1]
        for j in range(tiles):
            moved = field_u[c, j, own, :] - state[c, j, own, :] - 0.5 * scaled[c, j, own, :]
            moved = moved - x * applied[c, j, own, :] - y * intensity[c, j, own, :]
            momentum_out[c, :, pl.ds(j * LANES, LANES)] = moved * (1.0 / full(h[c])[:1])
    kick_hyper(STEPS, 0.5)

    out_row, out_col = sublane[:2, :2], lane[:2, :2]
    for high, low, ref in ((HYQ, HYE, hyper_out), (VEQ, VEE, velocity_out)):
        values = [[scal[base + c][:2, :2] for c in range(chains)] for base in (low, high)]
        pick = [jnp.where(out_col == 0, v[0], v[1]) for v in values]
        ref[...] = jnp.where(out_row == 0, pick[0], pick[1])

    def drain(k, carry):
        bulk(k).wait_send()
        return carry

    lax.fori_loop(0, STEPS + 1, drain, 0)


def hand_out(*refs):
    count = (len(refs) - 1) // 2
    sems = refs[-1]
    copies = [pltpu.make_async_copy(refs[i], refs[count + i], sems.at[i]) for i in range(count)]
    for copy in copies:
        copy.start()
    for copy in copies:
        copy.wait()


def solution(mesh):
    nr, nc = mesh.shape["row"], mesh.shape["col"]
    devices = nr * nc

    def shards(latent, momentum, hyper_params, velocity, step_size, counts, kappa_field):
        chains, rows, cols = latent.shape
        tiles = cols // LANES
        deep = rows + 2 * TOP
        total = float(rows * nr * cols * nc)
        sizes = (nr, nc, chains, rows, tiles, total)
        anywhere = pl.BlockSpec(memory_space=pltpu.HBM)
        small = pl.BlockSpec(memory_space=pltpu.VMEM)
        arrays = 2 * chains + 2
        f32 = jnp.float32
        fold_one, fold_two = LANES // (SEG * chains), LANES // (SEG * (chains + 2))
        everywhere = pltpu.VMEM((chains, tiles + 1, deep, LANES), f32)
        inner = pltpu.VMEM((chains, tiles, rows, LANES), f32)
        strip_one = pltpu.VMEM((2, rows // fold_one, LANES), f32)
        strip_two = pltpu.VMEM((2, rows // fold_two, LANES), f32)
        corner = pltpu.VMEM((2, 2, HALO, LANES), f32)
        results = pl.pallas_call(
            functools.partial(kernel, sizes),
            out_shape=(
                jax.ShapeDtypeStruct(latent.shape, f32),
                jax.ShapeDtypeStruct(latent.shape, f32),
                jax.ShapeDtypeStruct(hyper_params.shape, f32),
                jax.ShapeDtypeStruct(velocity.shape, f32),
            ),
            in_specs=[anywhere] * 7,
            out_specs=(small,) * 4,
            scratch_shapes=[
                pltpu.VMEM((arrays, tiles + 1, deep, LANES), f32),
                everywhere,
                pltpu.VMEM((tiles + 1, deep, LANES), f32),
                everywhere,
                everywhere,
                everywhere,
                inner,
                inner,
                pltpu.VMEM((tiles, rows, LANES), jnp.int32),
                everywhere,
                pltpu.VMEM((tiles, rows, LANES), f32),
                strip_one, strip_two, strip_one, strip_two, corner, corner,
                pltpu.VMEM((STEPS + 1, 1, LANES), f32),
                pltpu.VMEM((STEPS + 1, devices, 1, LANES), f32),
                pltpu.VMEM(((6 + COEFS) * chains + 1, 8, LANES), f32),
                pltpu.SMEM(hyper_params.shape, f32),
                pltpu.SMEM(velocity.shape, f32),
                pltpu.SMEM(step_size.shape, f32),
                pltpu.SemaphoreType.DMA((2 * tiles * (chains + 1) + 3,)),
                pltpu.SemaphoreType.DMA((16,)),
                pltpu.SemaphoreType.DMA((16,)),
                pltpu.SemaphoreType.DMA((STEPS + 1,)),
                pltpu.SemaphoreType.DMA((STEPS + 1,)),
                pltpu.SemaphoreType.REGULAR((len(signal_rounds(nr)),)),
            ],
            compiler_params=pltpu.CompilerParams(
                collective_id=0, has_side_effects=True, vmem_limit_bytes=24 * 1024 * 1024
            ),
        )(*(pltpu.with_memory_space_constraint(x, pltpu.HBM) for x in (
            latent, momentum, counts, kappa_field, hyper_params, velocity, step_size
        )))
        return pl.pallas_call(
            hand_out,
            out_shape=[jax.ShapeDtypeStruct(x.shape, f32) for x in results],
            in_specs=[small] * 4,
            out_specs=[pl.BlockSpec(memory_space=pl.ANY)] * 4,
            scratch_shapes=[pltpu.SemaphoreType.DMA((4,))],
            compiler_params=pltpu.CompilerParams(vmem_limit_bytes=8 * 1024 * 1024),
        )(*results)

    placed = (
        P(None, "row", "col"),
        P(None, "row", "col"),
        P(),
        P(),
        P(),
        P("row", "col"),
        P("row", "col"),
    )
    return jax.shard_map(
        shards,
        mesh=mesh,
        in_specs=placed,
        out_specs=(P(None, "row", "col"), P(None, "row", "col"), P(), P()),
        check_vma=False,
    )
```

```python
import functools

import jax
import jax.numpy as jnp
from jax import lax
from jax.experimental import pallas as pl
from jax.experimental.pallas import tpu as pltpu
from jax.sharding import PartitionSpec as P

STEPS = 10
HALO = 16
EDGE = 8
NEEDED = STEPS + 1
PAD = 8
TOP = PAD + HALO
LANES = 128
SEG = 16
MESH, LOGICAL = pl.DeviceIdType.MESH, pl.DeviceIdType.LOGICAL
COEFS = 6


def signal_rounds(nr):
    rounds, reach = [], 1
    while reach < nr // 2:
        rounds.append(reach)
        reach *= 2
    return rounds


def kernel(
    sizes, latent, momentum, counts, kappa, hyper_in, velocity_in, step_in,
    latent_out, momentum_out, hyper_out, velocity_out,
    state, field_u, diagonal, applied, intensity, scaled, scaled_applied, fresh, raw_counts,
    padded, half, pack_one, pack_two, take_one, take_two, corner_out, corner_in,
    payload, gathered, scal, hyper, velocity, step_size,
    load_sem, halo_send, halo_recv, sum_send, sum_recv, round_sem,
):
    nr, nc, chains, rows, tiles, total = sizes
    devices = nr * nc
    row, col = lax.axis_index("row"), lax.axis_index("col")
    me = row * nc + col
    kap, cnt = 2 * chains, 2 * chains + 1
    fold_one, fold_two = LANES // (SEG * chains), LANES // (SEG * (chains + 2))
    rows_one, rows_two = rows // fold_one, rows // fold_two
    own = pl.ds(TOP, rows)
    everything = range(tiles + 1)

    smalls = [(hyper_in, hyper), (velocity_in, velocity), (step_in, step_size)]
    vloads, loads = [], []
    for c in range(chains):
        for j in range(tiles):
            cols = pl.ds(j * LANES, LANES)
            vloads.append((latent.at[c, :, cols], state.at[c, j, own, :]))
            loads.append((momentum.at[c, :, cols], state.at[chains + c, j, own, :]))
    for j in range(tiles):
        cols = pl.ds(j * LANES, LANES)
        loads.append((kappa.at[:, cols], state.at[kap, j, own, :]))
        loads.append((counts.at[:, cols], raw_counts.at[j]))
    first_loads = len(vloads)
    loads = [
        pltpu.make_async_copy(s, d, load_sem.at[i]) for i, (s, d) in enumerate(vloads + loads + smalls)
    ]
    for copy in loads:
        copy.start()

    def wrap(d):
        other = me + d % devices
        return jnp.where(other < devices, other, other - devices)

    def at(dr, dc):
        return (lax.rem(row + (dr + nr), nr), lax.rem(col + (dc + nc), nc))

    barrier = pltpu.get_barrier_semaphore()
    near = [lax.rem(row + r, nr) * nc + c for r in (1, nr - 1) for c in range(nc)]
    near += [row * nc + jnp.where(col + c < nc, col + c, col + c - nc) for c in range(1, nc)]
    for other in near:
        pl.semaphore_signal(barrier, inc=1, device_id=other, device_id_type=LOGICAL)
    others = [wrap(d) for d in sorted(range(1, devices), key=lambda d: -min(d, devices - d))]

    lane = lax.broadcasted_iota(jnp.int32, (8, LANES), 1)
    sublane = lax.broadcasted_iota(jnp.int32, (8, LANES), 0)
    lane_row = lax.broadcasted_iota(jnp.int32, (1, LANES), 1)
    seg = lane_row // SEG
    first, last = lane_row == 0, lane_row == LANES - 1

    def fold(x):
        return sum(x[8 * i : 8 * i + 8] for i in range(x.shape[0] // 8))

    def whole(x):
        return jnp.broadcast_to(jnp.sum(jnp.sum(x, axis=0, keepdims=True), axis=1, keepdims=True), (8, LANES))

    def pack(ref, arrays, depth, folds):
        heads = tails = None
        for s in range(folds):
            part = pl.ds(TOP + s * depth, depth)
            for i, a in enumerate(arrays):
                slot = s * len(arrays) + i
                head, tail = state[a, 0, part, :], state[a, tiles - 1, part, :]
                if slot:
                    head = pltpu.roll(head, slot * SEG, 1)
                tail = pltpu.roll(tail, (slot + 1) * SEG % LANES, 1) if (slot + 1) * SEG % LANES else tail
                heads = head if heads is None else jnp.where(seg == slot, head, heads)
                tails = tail if tails is None else jnp.where(seg == slot, tail, tails)
        ref[0] = heads
        ref[1] = tails

    def unpack(right, left, slot_right, slot_left):
        turn = (LANES - SEG * slot_right) % LANES
        right = pltpu.roll(right, turn, 1) if turn else right
        turn = (LANES - SEG - SEG * slot_left) % LANES
        left = pltpu.roll(left, turn, 1) if turn else left
        return jnp.where(seg == 0, right, jnp.where(seg == LANES // SEG - 1, left, 0.0))

    for copy in loads[:first_loads]:
        copy.wait()
    pack(pack_one, list(range(chains)), rows_one, fold_one)
    pl.semaphore_wait(barrier, len(near))

    remotes = []

    def remote(src, dst, where):
        copy = pltpu.make_async_remote_copy(
            src_ref=src, dst_ref=dst, send_sem=halo_send.at[len(remotes)], recv_sem=halo_recv.at[len(remotes)],
            device_id=where, device_id_type=MESH,
        )
        remotes.append(copy)
        copy.start()

    vs = pl.ds(0, chains)
    flat = pl.ds(0, tiles)

    def rowcopies(arrays, near_row, depth):
        remote(
            state.at[arrays, flat, pl.ds(TOP + near_row, depth), :],
            state.at[arrays, flat, pl.ds(TOP + rows + near_row, depth), :],
            at(-1, 0),
        )
        remote(
            state.at[arrays, flat, pl.ds(TOP + rows - near_row - depth, depth), :],
            state.at[arrays, flat, pl.ds(TOP - near_row - depth, depth), :],
            at(1, 0),
        )

    remote(pack_one.at[0], take_one.at[0], at(0, -1))
    remote(pack_one.at[1], take_one.at[1], at(0, 1))
    rowcopies(vs, 0, EDGE)
    stage_one = len(remotes)

    rounds = signal_rounds(nr)

    def tell(i):
        for r in (rounds[i], -rounds[i]):
            pl.semaphore_signal(round_sem.at[i], inc=1, device_id=at(r, 0), device_id_type=MESH)

    tell(0)

    for copy in loads[first_loads:]:
        copy.wait()
    counted = jnp.zeros((8, LANES), jnp.float32)
    for j in range(tiles):
        value = raw_counts[j].astype(jnp.float32)
        state[cnt, j, own, :] = value
        counted += fold(value)
    for vert, start in ((1, TOP), (0, TOP + rows - HALO)):
        heads = tails = None
        for a in range(2 * chains + 2):
            head = state[a, 0, pl.ds(start, HALO), :]
            tail = pltpu.roll(state[a, tiles - 1, pl.ds(start, HALO), :], (a + 1) * SEG % LANES, 1)
            if a:
                head = pltpu.roll(head, a * SEG, 1)
            heads = head if heads is None else jnp.where(seg == a, head, heads)
            tails = tail if tails is None else jnp.where(seg == a, tail, tails)
        corner_out[0, vert] = heads
        corner_out[1, vert] = tails
    rest = pl.ds(chains, chains + 2)
    rowcopies(rest, 0, 1)
    for side, dc in ((0, -1), (1, 1)):
        for vert, dr in ((1, -1), (0, 1)):
            part = pl.ds(0 if vert else HALO - NEEDED, NEEDED)
            remote(corner_out.at[side, vert, part], corner_in.at[side, vert, part], at(dr, dc))
    early = remotes[stage_one:]
    rowcopies(rest, 1, NEEDED - 2)
    rowcopies(vs, EDGE, NEEDED - EDGE)
    bulk_rows = remotes[stage_one + len(early) :]
    pack(pack_two, list(range(chains, 2 * chains + 2)), rows_two, fold_two)
    remote(pack_two.at[0], take_two.at[0], at(0, -1))
    remote(pack_two.at[1], take_two.at[1], at(0, 1))
    early += remotes[-2:]

    h = [step_size[c] for c in range(chains)]
    hh = [h[c] * h[c] for c in range(chains)]

    def full(value):
        return jnp.full((8, LANES), value, jnp.float32)

    TAU, EXO, HYQ, HYE, VEQ, VEE = (i * chains for i in range(6))
    CO = 6 * chains
    LOCAL = CO + COEFS * chains
    for c in range(chains):
        scal[HYQ + c] = full(hyper[1, c])
        scal[HYE + c] = full(hyper[0, c])
        scal[VEQ + c] = full(velocity[1, c])
        scal[VEE + c] = full(velocity[0, c])
        scal[TAU + c] = jnp.exp(full(hyper[1, c]))
        scal[EXO + c] = jnp.exp(full(hyper[0, c]))
    scal[LOCAL] = whole(counted)

    mass = []
    for c in range(chains):
        acc = None
        for j in range(tiles):
            value = jnp.exp(state[c, j, own, :])
            intensity[c, j, own, :] = value
            acc = fold(value) if acc is None else acc + fold(value)
        mass.append(whole(acc))
    for j in range(tiles):
        diag = state[kap, j, own, :] + 4.0
        diagonal[j, own, :] = diag
        half[j] = 0.5 * diag
        for c in range(chains):
            hc = hh[c] * state[cnt, j, own, :]
            scaled[c, j, own, :] = hc
            field_u[c, j, own, :] = state[c, j, own, :] + (h[c] * state[chains + c, j, own, :] + 0.5 * hc)

    def stencil(ref, c, r, deep, lane_tiles):
        rowset = pl.ds(r, deep)
        at_tile = [ref[c, j, rowset, :] for j in everything]
        n = tiles + 1
        used = sorted({(j + s) % n for j in lane_tiles for s in (-1, 0)})
        to_right = {j: pltpu.roll(at_tile[j], 1, 1) for j in used}
        used = sorted({(j + s) % n for j in lane_tiles for s in (1, 0)})
        to_left = {j: pltpu.roll(at_tile[j], LANES - 1, 1) for j in used}
        out = []
        for j in lane_tiles:
            beside = jnp.where(first, to_right[(j - 1) % n], to_right[j])
            beside += jnp.where(last, to_left[(j + 1) % n], to_left[j])
            beside += ref[c, j, pl.ds(r - 1, deep), :] + ref[c, j, pl.ds(r + 1, deep), :]
            out.append((j, at_tile[j], diagonal[j, rowset, :] * at_tile[j] - beside))
        return out

    def half_stencil(ref, c, r, deep):
        rowset = pl.ds(r, deep)
        at_tile = [ref[c, j, rowset, :] for j in everything]
        to_left = [pltpu.roll(x, LANES - 1, 1) for x in at_tile]
        out = []
        for j in range(tiles):
            beside = jnp.where(last, to_left[j + 1], to_left[j]) + ref[c, j, pl.ds(r + 1, deep), :]
            out.append((j, at_tile[j], half[j, pl.ds(r - TOP, deep), :] * at_tile[j] - beside))
        return out

    DEEP = 64

    def own_blocks():
        return [TOP + i * DEEP for i in range(rows // DEEP)]

    def flanks():
        return [(r, DEEP, [tiles]) for r in own_blocks()]

    def ends():
        return [(PAD, HALO, everything), (TOP + rows, HALO, everything)]

    def sides():
        return flanks() + ends()

    def own_applied(ref):
        quads = []
        for c in range(chains):
            acc = jnp.zeros((8, LANES), jnp.float32)
            for r in own_blocks():
                for j, v, av in stencil(ref, c, r, DEEP, range(tiles)):
                    applied[c, j, pl.ds(r, DEEP), :] = av
                    acc += fold(v * av)
            quads.append(acc)
        return quads

    def halo_applied(regions):
        for c in range(chains):
            for r, deep, lane_tiles in regions:
                for j, _, av in stencil(state, c, r, deep, lane_tiles):
                    applied[c, j, pl.ds(r, deep), :] = av

    def send(k, quad, mass):
        out = scal[LOCAL][:1]
        for i, value in enumerate(quad + mass):
            out = jnp.where(seg == i, value[:1], out)
        payload[k] = out
        gathered[k, me] = out
        for other in others:
            pltpu.make_async_remote_copy(
                src_ref=payload.at[k], dst_ref=gathered.at[k, me],
                send_sem=sum_send.at[k], recv_sem=sum_recv.at[k],
                device_id=other, device_id_type=LOGICAL,
            ).start()

    def bulk(k):
        ref = gathered.at[k, pl.ds(0, devices - 1)]
        return pltpu.make_async_remote_copy(
            src_ref=ref, dst_ref=ref, send_sem=sum_send.at[k], recv_sem=sum_recv.at[k],
            device_id=others[0], device_id_type=LOGICAL,
        )

    def collect(k):
        bulk(k).wait_recv()
        summed = jnp.broadcast_to(jnp.sum(gathered[k], axis=0), (8, LANES))
        values = [
            jnp.broadcast_to(jnp.sum(jnp.where(lane == i * SEG, summed, 0.0), axis=1, keepdims=True), (8, LANES))
            for i in range(2 * chains + 1)
        ]
        return values[:chains], values[chains : 2 * chains], values[2 * chains]

    def kick_hyper(k, part):
        quad, mass, number = collect(k)
        for c in range(chains):
            aq = (0.5 / total) * (scal[TAU + c] * quad[c]) - 0.5
            ae = (scal[EXO + c] * mass[c] - number) * (1.0 / total)
            scal[VEQ + c] = scal[VEQ + c] - (part * h[c]) * aq
            scal[VEE + c] = scal[VEE + c] - (part * h[c]) * ae

    def drift_hyper():
        for c in range(chains):
            q = scal[HYQ + c] + h[c] * scal[VEQ + c]
            e = scal[HYE + c] + h[c] * scal[VEE + c]
            scal[HYQ + c] = q
            scal[HYE + c] = e
            scal[TAU + c] = jnp.exp(q)
            scal[EXO + c] = jnp.exp(e)

    def weights(part):
        xs = [(part * hh[c]) * scal[TAU + c] for c in range(chains)]
        ys = [(part * hh[c]) * scal[EXO + c] for c in range(chains)]
        return xs, ys

    def own_fresh(xs, ys):
        out = []
        for c in range(chains):
            x, y = xs[c][:1], ys[c][:1]
            acc = jnp.zeros((8, LANES), jnp.float32)
            for j in range(tiles):
                v = field_u[c, j, own, :] - x * applied[c, j, own, :] - y * intensity[c, j, own, :]
                value = jnp.exp(v)
                fresh[c, j] = v
                intensity[c, j, own, :] = value
                acc += fold(value)
            out.append(acc)
        return [whole(acc) for acc in out]

    def own_settle():
        for c in range(chains):
            for j in range(tiles):
                v = fresh[c, j]
                field_u[c, j, own, :] = (v + v) - state[c, j, own, :] + scaled[c, j, own, :]
                state[c, j, own, :] = v

    def halo_advance(xs, ys):
        for c in range(chains):
            x, y = xs[c][:1], ys[c][:1]
            for r, deep, lane_tiles in sides():
                rowset = pl.ds(r, deep)
                for j in lane_tiles:
                    v = field_u[c, j, rowset, :] - x * applied[c, j, rowset, :] - y * intensity[c, j, rowset, :]
                    field_u[c, j, rowset, :] = (v + v) - state[c, j, rowset, :] + scaled[c, j, rowset, :]
                    intensity[c, j, rowset, :] = jnp.exp(v)
                    state[c, j, rowset, :] = v

    def own_coefs(direct):
        for c in range(chains):
            sums = [jnp.zeros((8, LANES), jnp.float32)] * COEFS
            if not direct:
                for r in own_blocks():
                    rowset = pl.ds(r, DEEP)
                    for j, v, av in stencil(state, c, r, DEEP, range(tiles)):
                        au = (av + av) - applied[c, j, rowset, :] + scaled_applied[c, j, pl.ds(r - TOP, DEEP), :]
                        applied[c, j, rowset, :] = av
                        sums[0] += fold(field_u[c, j, rowset, :] * au)
                        sums[1] += fold(av * au)
                        sums[2] += fold(intensity[c, j, rowset, :] * au)
            yield c, sums

    def finish_coefs(direct, c, sums):
        for r in own_blocks():
            rowset = pl.ds(r, DEEP)
            if direct:
                for j, u, au in stencil(field_u, c, r, DEEP, range(tiles)):
                    sums[0] += fold(u * au)
                    sums[1] += fold(applied[c, j, rowset, :] * au)
                    sums[2] += fold(intensity[c, j, rowset, :] * au)
            for (j, a, ta), (_, e, te) in zip(half_stencil(applied, c, r, DEEP), half_stencil(intensity, c, r, DEEP)):
                sums[3] += fold(a * ta)
                sums[4] += fold(e * ta + a * te)
                sums[5] += fold(e * te)
        for i in range(COEFS):
            total_i = whole(sums[i])
            scal[CO + COEFS * c + i] = total_i + total_i if i in (3, 5) else total_i

    def predicted(xs, ys):
        out = []
        for c in range(chains):
            k0, k1, k2, k3, k4, k5 = [scal[CO + COEFS * c + i] for i in range(COEFS)]
            x, y = xs[c], ys[c]
            out.append(k0 - 2.0 * (x * k1 + y * k2) + (x * (x * k3 + 2.0 * (y * k4)) + y * (y * k5)))
        return out

    for c in range(chains):
        for r in (TOP - 8, TOP + rows):
            for j in range(tiles):
                padded[c, j, pl.ds(r, 8), :] = jnp.zeros((8, LANES), jnp.float32)
        padded[c, tiles, own, :] = jnp.zeros((rows, LANES), jnp.float32)
        for j in range(tiles):
            padded[c, j, own, :] = state[c, j, own, :]
    quad = own_applied(padded)
    place = lane_row % SEG

    for i in range(len(rounds)):
        pl.semaphore_wait(round_sem.at[i], 2)
        if i + 1 < len(rounds):
            tell(i + 1)
    for copy in remotes[:stage_one]:
        copy.wait_recv()
    across = jnp.where(place == SEG - 1, pack_one[1] * pltpu.roll(take_one[0], SEG - 1, 1), 0.0)
    across += jnp.where(place == 0, pack_one[0] * pltpu.roll(take_one[1], LANES - SEG + 1, 1), 0.0)
    across = fold(across)
    for c in range(chains):
        along = sum(
            state[c, j, pl.ds(TOP, 1), :] * state[c, j, pl.ds(TOP - 1, 1), :]
            + state[c, j, pl.ds(TOP + rows - 1, 1), :] * state[c, j, pl.ds(TOP + rows, 1), :]
            for j in range(tiles)
        )
        quad[c] = whole(quad[c] - jnp.where(seg % chains == c, across, 0.0) - jnp.where(sublane == 0, along, 0.0))
    send(0, quad, mass)

    for c in range(chains):
        for s in range(fold_one):
            slot = s * chains + c
            part = pl.ds(TOP + s * rows_one, rows_one)
            side = unpack(take_one[0], take_one[1], slot, slot)
            state[c, tiles, part, :] = side
            applied[c, 0, part, :] = applied[c, 0, part, :] - jnp.where(first, pltpu.roll(side, 1, 1), 0.0)
            applied[c, tiles - 1, part, :] = applied[c, tiles - 1, part, :] - jnp.where(
                last, pltpu.roll(side, LANES - 1, 1), 0.0
            )
        for j in range(tiles):
            for here, there in ((TOP, TOP - 1), (TOP + rows - 1, TOP + rows)):
                here, there = pl.ds(here, 1), pl.ds(there, 1)
                applied[c, j, here, :] = applied[c, j, here, :] - state[c, j, there, :]

    xs, ys = weights(0.5)
    mass = own_fresh(xs, ys)

    for copy in early:
        copy.wait_recv()
    for s in range(fold_two):
        for i in range(chains + 2):
            slot = s * (chains + 2) + i
            state[chains + i, tiles, pl.ds(TOP + s * rows_two, rows_two), :] = unpack(
                take_two[0], take_two[1], slot, slot
            )
    for vert, r in ((0, PAD), (1, TOP + rows)):
        for a in range(2 * chains + 2):
            state[a, tiles, pl.ds(r, HALO), :] = unpack(corner_in[0, vert], corner_in[1, vert], a, a)
    def halo_start(regions):
        for r, deep, lane_tiles in regions:
            rowset = pl.ds(r, deep)
            for j in lane_tiles:
                diagonal[j, rowset, :] = state[kap, j, rowset, :] + 4.0
                for c in range(chains):
                    hc = hh[c] * state[cnt, j, rowset, :]
                    scaled[c, j, rowset, :] = hc
                    v = state[c, j, rowset, :]
                    intensity[c, j, rowset, :] = jnp.exp(v)
                    field_u[c, j, rowset, :] = v + (h[c] * state[chains + c, j, rowset, :] + 0.5 * hc)

    halo_start(flanks())
    halo_applied(flanks())
    for c in range(chains):
        x, y = xs[c][:1], ys[c][:1]
        padded[c, tiles, own, :] = (
            field_u[c, tiles, own, :] - x * applied[c, tiles, own, :] - y * intensity[c, tiles, own, :]
        )
        for r in (TOP - 1, TOP + rows):
            line = pl.ds(r, 1)
            cells = [state[c, j, line, :] for j in everything]
            to_right, to_left = [pltpu.roll(z, 1, 1) for z in cells], [pltpu.roll(z, LANES - 1, 1) for z in cells]
            for j in range(tiles):
                beside = jnp.where(first, to_right[(j - 1) % (tiles + 1)], to_right[j])
                beside += jnp.where(last, to_left[j + 1], to_left[j])
                beside += state[c, j, pl.ds(r - 1, 1), :] + state[c, j, pl.ds(r + 1, 1), :]
                av = (state[kap, j, line, :] + 4.0) * cells[j] - beside
                u = cells[j] + (h[c] * state[chains + c, j, line, :] + 0.5 * (hh[c] * state[cnt, j, line, :]))
                padded[c, j, line, :] = u - x * av - y * jnp.exp(cells[j])
        for j in range(tiles):
            padded[c, j, own, :] = fresh[c, j]
    send(1, [whole(q) for q in own_applied(padded)], mass)

    for copy in bulk_rows:
        copy.wait_recv()
    for copy in remotes:
        copy.wait_send()
    halo_start(ends())
    halo_applied(ends())
    halo_advance(xs, ys)
    own_settle()
    halo_applied(sides())
    for r in own_blocks():
        for j, _, value in stencil(state, cnt, r, DEEP, range(tiles)):
            for c in range(chains):
                scaled_applied[c, j, pl.ds(r - TOP, DEEP), :] = hh[c] * value
    for c, sums in own_coefs(True):
        finish_coefs(True, c, sums)

    def step(k, carry):
        kick_hyper(k - 1, jnp.where(k == 1, 0.5, 1.0))
        drift_hyper()
        xs, ys = weights(1.0)
        mass = own_fresh(xs, ys)
        send(k + 1, predicted(xs, ys), mass)
        halo_advance(xs, ys)
        own_settle()
        pairs = list(own_coefs(False))
        halo_applied(sides())
        for c, sums in pairs:
            finish_coefs(False, c, sums)
        return carry

    lax.fori_loop(1, STEPS, step, 0)

    for c in range(chains):
        for j in range(tiles):
            latent_out[c, :, pl.ds(j * LANES, LANES)] = state[c, j, own, :]
    kick_hyper(STEPS - 1, 1.0)
    drift_hyper()
    xs, ys = weights(0.5)
    for c in range(chains):
        x, y = xs[c][:1], ys[c][:1]
        for j in range(tiles):
            moved = field_u[c, j, own, :] - state[c, j, own, :] - 0.5 * scaled[c, j, own, :]
            moved = moved - x * applied[c, j, own, :] - y * intensity[c, j, own, :]
            momentum_out[c, :, pl.ds(j * LANES, LANES)] = moved * (1.0 / full(h[c])[:1])
    kick_hyper(STEPS, 0.5)

    out_row, out_col = sublane[:2, :2], lane[:2, :2]
    for high, low, ref in ((HYQ, HYE, hyper_out), (VEQ, VEE, velocity_out)):
        values = [[scal[base + c][:2, :2] for c in range(chains)] for base in (low, high)]
        pick = [jnp.where(out_col == 0, v[0], v[1]) for v in values]
        ref[...] = jnp.where(out_row == 0, pick[0], pick[1])

    def drain(k, carry):
        bulk(k).wait_send()
        return carry

    lax.fori_loop(0, STEPS + 1, drain, 0)


def hand_out(*refs):
    count = (len(refs) - 1) // 2
    sems = refs[-1]
    copies = [pltpu.make_async_copy(refs[i], refs[count + i], sems.at[i]) for i in range(count)]
    for copy in copies:
        copy.start()
    for copy in copies:
        copy.wait()


def solution(mesh):
    nr, nc = mesh.shape["row"], mesh.shape["col"]
    devices = nr * nc

    def shards(latent, momentum, hyper_params, velocity, step_size, counts, kappa_field):
        chains, rows, cols = latent.shape
        tiles = cols // LANES
        deep = rows + 2 * TOP
        total = float(rows * nr * cols * nc)
        sizes = (nr, nc, chains, rows, tiles, total)
        anywhere = pl.BlockSpec(memory_space=pltpu.HBM)
        small = pl.BlockSpec(memory_space=pltpu.VMEM)
        arrays = 2 * chains + 2
        f32 = jnp.float32
        fold_one, fold_two = LANES // (SEG * chains), LANES // (SEG * (chains + 2))
        everywhere = pltpu.VMEM((chains, tiles + 1, deep, LANES), f32)
        inner = pltpu.VMEM((chains, tiles, rows, LANES), f32)
        strip_one = pltpu.VMEM((2, rows // fold_one, LANES), f32)
        strip_two = pltpu.VMEM((2, rows // fold_two, LANES), f32)
        corner = pltpu.VMEM((2, 2, HALO, LANES), f32)
        results = pl.pallas_call(
            functools.partial(kernel, sizes),
            out_shape=(
                jax.ShapeDtypeStruct(latent.shape, f32),
                jax.ShapeDtypeStruct(latent.shape, f32),
                jax.ShapeDtypeStruct(hyper_params.shape, f32),
                jax.ShapeDtypeStruct(velocity.shape, f32),
            ),
            in_specs=[anywhere] * 7,
            out_specs=(small,) * 4,
            scratch_shapes=[
                pltpu.VMEM((arrays, tiles + 1, deep, LANES), f32),
                everywhere,
                pltpu.VMEM((tiles + 1, deep, LANES), f32),
                everywhere,
                everywhere,
                everywhere,
                inner,
                inner,
                pltpu.VMEM((tiles, rows, LANES), jnp.int32),
                everywhere,
                pltpu.VMEM((tiles, rows, LANES), f32),
                strip_one, strip_two, strip_one, strip_two, corner, corner,
                pltpu.VMEM((STEPS + 1, 1, LANES), f32),
                pltpu.VMEM((STEPS + 1, devices, 1, LANES), f32),
                pltpu.VMEM(((6 + COEFS) * chains + 1, 8, LANES), f32),
                pltpu.SMEM(hyper_params.shape, f32),
                pltpu.SMEM(velocity.shape, f32),
                pltpu.SMEM(step_size.shape, f32),
                pltpu.SemaphoreType.DMA((2 * tiles * (chains + 1) + 3,)),
                pltpu.SemaphoreType.DMA((16,)),
                pltpu.SemaphoreType.DMA((16,)),
                pltpu.SemaphoreType.DMA((STEPS + 1,)),
                pltpu.SemaphoreType.DMA((STEPS + 1,)),
                pltpu.SemaphoreType.REGULAR((len(signal_rounds(nr)),)),
            ],
            compiler_params=pltpu.CompilerParams(
                collective_id=0, has_side_effects=True, vmem_limit_bytes=24 * 1024 * 1024
            ),
        )(*(pltpu.with_memory_space_constraint(x, pltpu.HBM) for x in (
            latent, momentum, counts, kappa_field, hyper_params, velocity, step_size
        )))
        return pl.pallas_call(
            hand_out,
            out_shape=[jax.ShapeDtypeStruct(x.shape, f32) for x in results],
            in_specs=[small] * 4,
            out_specs=[pl.BlockSpec(memory_space=pl.ANY)] * 4,
            scratch_shapes=[pltpu.SemaphoreType.DMA((4,))],
            compiler_params=pltpu.CompilerParams(vmem_limit_bytes=8 * 1024 * 1024),
        )(*results)

    placed = (
        P(None, "row", "col"),
        P(None, "row", "col"),
        P(),
        P(),
        P(),
        P("row", "col"),
        P("row", "col"),
    )
    return jax.shard_map(
        shards,
        mesh=mesh,
        in_specs=placed,
        out_specs=(P(None, "row", "col"), P(None, "row", "col"), P(), P()),
        check_vma=False,
    )
```

```python
import functools

import jax
import jax.numpy as jnp
from jax import lax
from jax.experimental import pallas as pl
from jax.experimental.pallas import tpu as pltpu
from jax.sharding import PartitionSpec as P

STEPS = 10
HALO = 16
EDGE = 8
NEEDED = STEPS + 1
PAD = 8
TOP = PAD + HALO
LANES = 128
SEG = 16
MESH, LOGICAL = pl.DeviceIdType.MESH, pl.DeviceIdType.LOGICAL
COEFS = 6


def signal_rounds(nr):
    rounds, reach = [], 1
    while reach < nr // 2:
        rounds.append(reach)
        reach *= 2
    return rounds


def kernel(
    sizes, latent, momentum, counts, kappa, hyper_in, velocity_in, step_in,
    latent_out, momentum_out, hyper_out, velocity_out,
    state, field_u, diagonal, applied, intensity, scaled, scaled_applied, fresh, raw_counts,
    padded, half, pack_one, pack_two, take_one, take_two, corner_out, corner_in,
    payload, gathered, scal, hyper, velocity, step_size,
    load_sem, halo_send, halo_recv, sum_send, sum_recv, round_sem,
):
    nr, nc, chains, rows, tiles, total = sizes
    devices = nr * nc
    row, col = lax.axis_index("row"), lax.axis_index("col")
    me = row * nc + col
    kap, cnt = 2 * chains, 2 * chains + 1
    fold_one, fold_two = LANES // (SEG * chains), LANES // (SEG * (chains + 2))
    rows_one, rows_two = rows // fold_one, rows // fold_two
    own = pl.ds(TOP, rows)
    everything = range(tiles + 1)

    smalls = [(hyper_in, hyper), (velocity_in, velocity), (step_in, step_size)]
    vloads, loads = [], []
    for c in range(chains):
        for j in range(tiles):
            cols = pl.ds(j * LANES, LANES)
            vloads.append((latent.at[c, :, cols], state.at[c, j, own, :]))
            loads.append((momentum.at[c, :, cols], state.at[chains + c, j, own, :]))
    for j in range(tiles):
        cols = pl.ds(j * LANES, LANES)
        loads.append((kappa.at[:, cols], state.at[kap, j, own, :]))
        loads.append((counts.at[:, cols], raw_counts.at[j]))
    first_loads = len(vloads)
    loads = [
        pltpu.make_async_copy(s, d, load_sem.at[i]) for i, (s, d) in enumerate(vloads + loads + smalls)
    ]
    for copy in loads:
        copy.start()

    def wrap(d):
        other = me + d % devices
        return jnp.where(other < devices, other, other - devices)

    def flip(x, mask):
        bits = [b for b in (1 << i for i in range(mask.bit_length())) if mask & b]
        return x + sum(b - 2 * b * (x // b % 2) for b in bits)

    def at(dr, dc):
        return (lax.rem(row + (dr + nr), nr), lax.rem(col + (dc + nc), nc))

    barrier = pltpu.get_barrier_semaphore()
    near = [lax.rem(row + r, nr) * nc + c for r in (1, nr - 1) for c in range(nc)]
    near += [row * nc + jnp.where(col + c < nc, col + c, col + c - nc) for c in range(1, nc)]
    for other in near:
        pl.semaphore_signal(barrier, inc=1, device_id=other, device_id_type=LOGICAL)
    if nr & (nr - 1) or nc & (nc - 1):
        others = [wrap(d) for d in range(1, devices)]
    else:
        pairs = [(r, c) for r in range(nr) for c in range(nc) if r or c]
        pairs.sort(key=lambda p: (p[1] & 1) - 2 * (p[0] + bin(p[1] >> 1).count("1")))
        others = [flip(row, r) * nc + flip(col, c) for r, c in pairs]

    lane = lax.broadcasted_iota(jnp.int32, (8, LANES), 1)
    sublane = lax.broadcasted_iota(jnp.int32, (8, LANES), 0)
    lane_row = lax.broadcasted_iota(jnp.int32, (1, LANES), 1)
    seg = lane_row // SEG
    first, last = lane_row == 0, lane_row == LANES - 1

    def fold(x):
        return sum(x[8 * i : 8 * i + 8] for i in range(x.shape[0] // 8))

    def whole(x):
        return jnp.broadcast_to(jnp.sum(jnp.sum(x, axis=0, keepdims=True), axis=1, keepdims=True), (8, LANES))

    def pack(ref, arrays, depth, folds):
        heads = tails = None
        for s in range(folds):
            part = pl.ds(TOP + s * depth, depth)
            for i, a in enumerate(arrays):
                slot = s * len(arrays) + i
                head, tail = state[a, 0, part, :], state[a, tiles - 1, part, :]
                if slot:
                    head = pltpu.roll(head, slot * SEG, 1)
                tail = pltpu.roll(tail, (slot + 1) * SEG % LANES, 1) if (slot + 1) * SEG % LANES else tail
                heads = head if heads is None else jnp.where(seg == slot, head, heads)
                tails = tail if tails is None else jnp.where(seg == slot, tail, tails)
        ref[0] = heads
        ref[1] = tails

    def unpack(right, left, slot_right, slot_left):
        turn = (LANES - SEG * slot_right) % LANES
        right = pltpu.roll(right, turn, 1) if turn else right
        turn = (LANES - SEG - SEG * slot_left) % LANES
        left = pltpu.roll(left, turn, 1) if turn else left
        return jnp.where(seg == 0, right, jnp.where(seg == LANES // SEG - 1, left, 0.0))

    for copy in loads[:first_loads]:
        copy.wait()
    pack(pack_one, list(range(chains)), rows_one, fold_one)
    pl.semaphore_wait(barrier, len(near))

    remotes = []

    def remote(src, dst, where):
        copy = pltpu.make_async_remote_copy(
            src_ref=src, dst_ref=dst, send_sem=halo_send.at[len(remotes)], recv_sem=halo_recv.at[len(remotes)],
            device_id=where, device_id_type=MESH,
        )
        remotes.append(copy)
        copy.start()

    vs = pl.ds(0, chains)
    flat = pl.ds(0, tiles)

    def rowcopies(arrays, near_row, depth):
        remote(
            state.at[arrays, flat, pl.ds(TOP + near_row, depth), :],
            state.at[arrays, flat, pl.ds(TOP + rows + near_row, depth), :],
            at(-1, 0),
        )
        remote(
            state.at[arrays, flat, pl.ds(TOP + rows - near_row - depth, depth), :],
            state.at[arrays, flat, pl.ds(TOP - near_row - depth, depth), :],
            at(1, 0),
        )

    remote(pack_one.at[0], take_one.at[0], at(0, -1))
    remote(pack_one.at[1], take_one.at[1], at(0, 1))
    rowcopies(vs, 0, EDGE)
    stage_one = len(remotes)

    rounds = signal_rounds(nr)

    def tell(i):
        for r in (rounds[i], -rounds[i]):
            pl.semaphore_signal(round_sem.at[i], inc=1, device_id=at(r, 0), device_id_type=MESH)

    tell(0)

    for copy in loads[first_loads:]:
        copy.wait()
    counted = jnp.zeros((8, LANES), jnp.float32)
    for j in range(tiles):
        value = raw_counts[j].astype(jnp.float32)
        state[cnt, j, own, :] = value
        counted += fold(value)
    for vert, start in ((1, TOP), (0, TOP + rows - HALO)):
        heads = tails = None
        for a in range(2 * chains + 2):
            head = state[a, 0, pl.ds(start, HALO), :]
            tail = pltpu.roll(state[a, tiles - 1, pl.ds(start, HALO), :], (a + 1) * SEG % LANES, 1)
            if a:
                head = pltpu.roll(head, a * SEG, 1)
            heads = head if heads is None else jnp.where(seg == a, head, heads)
            tails = tail if tails is None else jnp.where(seg == a, tail, tails)
        corner_out[0, vert] = heads
        corner_out[1, vert] = tails
    rest = pl.ds(chains, chains + 2)
    rowcopies(rest, 0, 1)
    for side, dc in ((0, -1), (1, 1)):
        for vert, dr in ((1, -1), (0, 1)):
            part = pl.ds(0 if vert else HALO - NEEDED, NEEDED)
            remote(corner_out.at[side, vert, part], corner_in.at[side, vert, part], at(dr, dc))
    early = remotes[stage_one:]
    rowcopies(rest, 1, NEEDED - 2)
    rowcopies(vs, EDGE, NEEDED - EDGE)
    bulk_rows = remotes[stage_one + len(early) :]
    pack(pack_two, list(range(chains, 2 * chains + 2)), rows_two, fold_two)
    remote(pack_two.at[0], take_two.at[0], at(0, -1))
    remote(pack_two.at[1], take_two.at[1], at(0, 1))
    early += remotes[-2:]

    h = [step_size[c] for c in range(chains)]
    hh = [h[c] * h[c] for c in range(chains)]

    def full(value):
        return jnp.full((8, LANES), value, jnp.float32)

    TAU, EXO, HYQ, HYE, VEQ, VEE = (i * chains for i in range(6))
    CO = 6 * chains
    LOCAL = CO + COEFS * chains
    for c in range(chains):
        scal[HYQ + c] = full(hyper[1, c])
        scal[HYE + c] = full(hyper[0, c])
        scal[VEQ + c] = full(velocity[1, c])
        scal[VEE + c] = full(velocity[0, c])
        scal[TAU + c] = jnp.exp(full(hyper[1, c]))
        scal[EXO + c] = jnp.exp(full(hyper[0, c]))
    scal[LOCAL] = whole(counted)

    mass = []
    for c in range(chains):
        acc = None
        for j in range(tiles):
            value = jnp.exp(state[c, j, own, :])
            intensity[c, j, own, :] = value
            acc = fold(value) if acc is None else acc + fold(value)
        mass.append(whole(acc))
    for j in range(tiles):
        diag = state[kap, j, own, :] + 4.0
        diagonal[j, own, :] = diag
        half[j] = 0.5 * diag
        for c in range(chains):
            hc = hh[c] * state[cnt, j, own, :]
            scaled[c, j, own, :] = hc
            field_u[c, j, own, :] = state[c, j, own, :] + (h[c] * state[chains + c, j, own, :] + 0.5 * hc)

    def stencil(ref, c, r, deep, lane_tiles):
        rowset = pl.ds(r, deep)
        at_tile = [ref[c, j, rowset, :] for j in everything]
        n = tiles + 1
        used = sorted({(j + s) % n for j in lane_tiles for s in (-1, 0)})
        to_right = {j: pltpu.roll(at_tile[j], 1, 1) for j in used}
        used = sorted({(j + s) % n for j in lane_tiles for s in (1, 0)})
        to_left = {j: pltpu.roll(at_tile[j], LANES - 1, 1) for j in used}
        out = []
        for j in lane_tiles:
            beside = jnp.where(first, to_right[(j - 1) % n], to_right[j])
            beside += jnp.where(last, to_left[(j + 1) % n], to_left[j])
            beside += ref[c, j, pl.ds(r - 1, deep), :] + ref[c, j, pl.ds(r + 1, deep), :]
            out.append((j, at_tile[j], diagonal[j, rowset, :] * at_tile[j] - beside))
        return out

    def half_stencil(ref, c, r, deep):
        rowset = pl.ds(r, deep)
        at_tile = [ref[c, j, rowset, :] for j in everything]
        to_left = [pltpu.roll(x, LANES - 1, 1) for x in at_tile]
        out = []
        for j in range(tiles):
            beside = jnp.where(last, to_left[j + 1], to_left[j]) + ref[c, j, pl.ds(r + 1, deep), :]
            out.append((j, at_tile[j], half[j, pl.ds(r - TOP, deep), :] * at_tile[j] - beside))
        return out

    DEEP = 64

    def own_blocks():
        return [TOP + i * DEEP for i in range(rows // DEEP)]

    def flanks():
        return [(r, DEEP, [tiles]) for r in own_blocks()]

    def ends():
        return [(PAD, HALO, everything), (TOP + rows, HALO, everything)]

    def sides():
        return flanks() + ends()

    def own_applied(ref):
        quads = []
        for c in range(chains):
            acc = jnp.zeros((8, LANES), jnp.float32)
            for r in own_blocks():
                for j, v, av in stencil(ref, c, r, DEEP, range(tiles)):
                    applied[c, j, pl.ds(r, DEEP), :] = av
                    acc += fold(v * av)
            quads.append(acc)
        return quads

    def halo_applied(regions):
        for c in range(chains):
            for r, deep, lane_tiles in regions:
                for j, _, av in stencil(state, c, r, deep, lane_tiles):
                    applied[c, j, pl.ds(r, deep), :] = av

    def send(k, quad, mass):
        out = scal[LOCAL][:1]
        for i, value in enumerate(quad + mass):
            out = jnp.where(seg == i, value[:1], out)
        payload[k] = out
        gathered[k, me] = out
        for other in others:
            pltpu.make_async_remote_copy(
                src_ref=payload.at[k], dst_ref=gathered.at[k, me],
                send_sem=sum_send.at[k], recv_sem=sum_recv.at[k],
                device_id=other, device_id_type=LOGICAL,
            ).start()

    def bulk(k):
        ref = gathered.at[k, pl.ds(0, devices - 1)]
        return pltpu.make_async_remote_copy(
            src_ref=ref, dst_ref=ref, send_sem=sum_send.at[k], recv_sem=sum_recv.at[k],
            device_id=others[0], device_id_type=LOGICAL,
        )

    def collect(k):
        bulk(k).wait_recv()
        summed = jnp.broadcast_to(jnp.sum(gathered[k], axis=0), (8, LANES))
        values = [
            jnp.broadcast_to(jnp.sum(jnp.where(lane == i * SEG, summed, 0.0), axis=1, keepdims=True), (8, LANES))
            for i in range(2 * chains + 1)
        ]
        return values[:chains], values[chains : 2 * chains], values[2 * chains]

    def kick_hyper(k, part):
        quad, mass, number = collect(k)
        for c in range(chains):
            aq = (0.5 / total) * (scal[TAU + c] * quad[c]) - 0.5
            ae = (scal[EXO + c] * mass[c] - number) * (1.0 / total)
            scal[VEQ + c] = scal[VEQ + c] - (part * h[c]) * aq
            scal[VEE + c] = scal[VEE + c] - (part * h[c]) * ae

    def drift_hyper():
        for c in range(chains):
            q = scal[HYQ + c] + h[c] * scal[VEQ + c]
            e = scal[HYE + c] + h[c] * scal[VEE + c]
            scal[HYQ + c] = q
            scal[HYE + c] = e
            scal[TAU + c] = jnp.exp(q)
            scal[EXO + c] = jnp.exp(e)

    def weights(part):
        xs = [(part * hh[c]) * scal[TAU + c] for c in range(chains)]
        ys = [(part * hh[c]) * scal[EXO + c] for c in range(chains)]
        return xs, ys

    def own_fresh(xs, ys):
        out = []
        for c in range(chains):
            x, y = xs[c][:1], ys[c][:1]
            acc = jnp.zeros((8, LANES), jnp.float32)
            for j in range(tiles):
                v = field_u[c, j, own, :] - x * applied[c, j, own, :] - y * intensity[c, j, own, :]
                value = jnp.exp(v)
                fresh[c, j] = v
                intensity[c, j, own, :] = value
                acc += fold(value)
            out.append(acc)
        return [whole(acc) for acc in out]

    def own_settle():
        for c in range(chains):
            for j in range(tiles):
                v = fresh[c, j]
                field_u[c, j, own, :] = (v + v) - state[c, j, own, :] + scaled[c, j, own, :]
                state[c, j, own, :] = v

    def halo_advance(xs, ys):
        for c in range(chains):
            x, y = xs[c][:1], ys[c][:1]
            for r, deep, lane_tiles in sides():
                rowset = pl.ds(r, deep)
                for j in lane_tiles:
                    v = field_u[c, j, rowset, :] - x * applied[c, j, rowset, :] - y * intensity[c, j, rowset, :]
                    field_u[c, j, rowset, :] = (v + v) - state[c, j, rowset, :] + scaled[c, j, rowset, :]
                    intensity[c, j, rowset, :] = jnp.exp(v)
                    state[c, j, rowset, :] = v

    def own_coefs(direct):
        for c in range(chains):
            sums = [jnp.zeros((8, LANES), jnp.float32)] * COEFS
            if not direct:
                for r in own_blocks():
                    rowset = pl.ds(r, DEEP)
                    for j, v, av in stencil(state, c, r, DEEP, range(tiles)):
                        au = (av + av) - applied[c, j, rowset, :] + scaled_applied[c, j, pl.ds(r - TOP, DEEP), :]
                        applied[c, j, rowset, :] = av
                        sums[0] += fold(field_u[c, j, rowset, :] * au)
                        sums[1] += fold(av * au)
                        sums[2] += fold(intensity[c, j, rowset, :] * au)
            yield c, sums

    def finish_coefs(direct, c, sums):
        for r in own_blocks():
            rowset = pl.ds(r, DEEP)
            if direct:
                for j, u, au in stencil(field_u, c, r, DEEP, range(tiles)):
                    sums[0] += fold(u * au)
                    sums[1] += fold(applied[c, j, rowset, :] * au)
                    sums[2] += fold(intensity[c, j, rowset, :] * au)
            for (j, a, ta), (_, e, te) in zip(half_stencil(applied, c, r, DEEP), half_stencil(intensity, c, r, DEEP)):
                sums[3] += fold(a * ta)
                sums[4] += fold(e * ta + a * te)
                sums[5] += fold(e * te)
        for i in range(COEFS):
            total_i = whole(sums[i])
            scal[CO + COEFS * c + i] = total_i + total_i if i in (3, 5) else total_i

    def predicted(xs, ys):
        out = []
        for c in range(chains):
            k0, k1, k2, k3, k4, k5 = [scal[CO + COEFS * c + i] for i in range(COEFS)]
            x, y = xs[c], ys[c]
            out.append(k0 - 2.0 * (x * k1 + y * k2) + (x * (x * k3 + 2.0 * (y * k4)) + y * (y * k5)))
        return out

    for c in range(chains):
        for r in (TOP - 8, TOP + rows):
            for j in range(tiles):
                padded[c, j, pl.ds(r, 8), :] = jnp.zeros((8, LANES), jnp.float32)
        padded[c, tiles, own, :] = jnp.zeros((rows, LANES), jnp.float32)
        for j in range(tiles):
            padded[c, j, own, :] = state[c, j, own, :]
    quad = own_applied(padded)
    place = lane_row % SEG

    for i in range(len(rounds)):
        pl.semaphore_wait(round_sem.at[i], 2)
        if i + 1 < len(rounds):
            tell(i + 1)
    for copy in remotes[:stage_one]:
        copy.wait_recv()
    across = jnp.where(place == SEG - 1, pack_one[1] * pltpu.roll(take_one[0], SEG - 1, 1), 0.0)
    across += jnp.where(place == 0, pack_one[0] * pltpu.roll(take_one[1], LANES - SEG + 1, 1), 0.0)
    across = fold(across)
    for c in range(chains):
        along = sum(
            state[c, j, pl.ds(TOP, 1), :] * state[c, j, pl.ds(TOP - 1, 1), :]
            + state[c, j, pl.ds(TOP + rows - 1, 1), :] * state[c, j, pl.ds(TOP + rows, 1), :]
            for j in range(tiles)
        )
        quad[c] = whole(quad[c] - jnp.where(seg % chains == c, across, 0.0) - jnp.where(sublane == 0, along, 0.0))
    send(0, quad, mass)

    for c in range(chains):
        for s in range(fold_one):
            slot = s * chains + c
            part = pl.ds(TOP + s * rows_one, rows_one)
            side = unpack(take_one[0], take_one[1], slot, slot)
            state[c, tiles, part, :] = side
            applied[c, 0, part, :] = applied[c, 0, part, :] - jnp.where(first, pltpu.roll(side, 1, 1), 0.0)
            applied[c, tiles - 1, part, :] = applied[c, tiles - 1, part, :] - jnp.where(
                last, pltpu.roll(side, LANES - 1, 1), 0.0
            )
        for j in range(tiles):
            for here, there in ((TOP, TOP - 1), (TOP + rows - 1, TOP + rows)):
                here, there = pl.ds(here, 1), pl.ds(there, 1)
                applied[c, j, here, :] = applied[c, j, here, :] - state[c, j, there, :]

    xs, ys = weights(0.5)
    mass = own_fresh(xs, ys)

    for copy in early:
        copy.wait_recv()
    for s in range(fold_two):
        for i in range(chains + 2):
            slot = s * (chains + 2) + i
            state[chains + i, tiles, pl.ds(TOP + s * rows_two, rows_two), :] = unpack(
                take_two[0], take_two[1], slot, slot
            )
    for vert, r in ((0, PAD), (1, TOP + rows)):
        for a in range(2 * chains + 2):
            state[a, tiles, pl.ds(r, HALO), :] = unpack(corner_in[0, vert], corner_in[1, vert], a, a)
    def halo_start(regions):
        for r, deep, lane_tiles in regions:
            rowset = pl.ds(r, deep)
            for j in lane_tiles:
                diagonal[j, rowset, :] = state[kap, j, rowset, :] + 4.0
                for c in range(chains):
                    hc = hh[c] * state[cnt, j, rowset, :]
                    scaled[c, j, rowset, :] = hc
                    v = state[c, j, rowset, :]
                    intensity[c, j, rowset, :] = jnp.exp(v)
                    field_u[c, j, rowset, :] = v + (h[c] * state[chains + c, j, rowset, :] + 0.5 * hc)

    halo_start(flanks())
    halo_applied(flanks())
    for c in range(chains):
        x, y = xs[c][:1], ys[c][:1]
        padded[c, tiles, own, :] = (
            field_u[c, tiles, own, :] - x * applied[c, tiles, own, :] - y * intensity[c, tiles, own, :]
        )
        for r in (TOP - 1, TOP + rows):
            line = pl.ds(r, 1)
            cells = [state[c, j, line, :] for j in everything]
            to_right, to_left = [pltpu.roll(z, 1, 1) for z in cells], [pltpu.roll(z, LANES - 1, 1) for z in cells]
            for j in range(tiles):
                beside = jnp.where(first, to_right[(j - 1) % (tiles + 1)], to_right[j])
                beside += jnp.where(last, to_left[j + 1], to_left[j])
                beside += state[c, j, pl.ds(r - 1, 1), :] + state[c, j, pl.ds(r + 1, 1), :]
                av = (state[kap, j, line, :] + 4.0) * cells[j] - beside
                u = cells[j] + (h[c] * state[chains + c, j, line, :] + 0.5 * (hh[c] * state[cnt, j, line, :]))
                padded[c, j, line, :] = u - x * av - y * jnp.exp(cells[j])
        for j in range(tiles):
            padded[c, j, own, :] = fresh[c, j]
    send(1, [whole(q) for q in own_applied(padded)], mass)

    for copy in bulk_rows:
        copy.wait_recv()
    for copy in remotes:
        copy.wait_send()
    halo_start(ends())
    halo_applied(ends())
    halo_advance(xs, ys)
    own_settle()
    halo_applied(sides())
    for r in own_blocks():
        for j, _, value in stencil(state, cnt, r, DEEP, range(tiles)):
            for c in range(chains):
                scaled_applied[c, j, pl.ds(r - TOP, DEEP), :] = hh[c] * value
    for c, sums in own_coefs(True):
        finish_coefs(True, c, sums)

    def step(k, carry):
        kick_hyper(k - 1, jnp.where(k == 1, 0.5, 1.0))
        drift_hyper()
        xs, ys = weights(1.0)
        mass = own_fresh(xs, ys)
        send(k + 1, predicted(xs, ys), mass)
        halo_advance(xs, ys)
        own_settle()
        pairs = list(own_coefs(False))
        halo_applied(sides())
        for c, sums in pairs:
            finish_coefs(False, c, sums)
        return carry

    lax.fori_loop(1, STEPS, step, 0)

    for c in range(chains):
        for j in range(tiles):
            latent_out[c, :, pl.ds(j * LANES, LANES)] = state[c, j, own, :]
    kick_hyper(STEPS - 1, 1.0)
    drift_hyper()
    xs, ys = weights(0.5)
    for c in range(chains):
        x, y = xs[c][:1], ys[c][:1]
        for j in range(tiles):
            moved = field_u[c, j, own, :] - state[c, j, own, :] - 0.5 * scaled[c, j, own, :]
            moved = moved - x * applied[c, j, own, :] - y * intensity[c, j, own, :]
            momentum_out[c, :, pl.ds(j * LANES, LANES)] = moved * (1.0 / full(h[c])[:1])
    out_row, out_col = sublane[:2, :2], lane[:2, :2]

    def show(high, low, ref):
        values = [[scal[base + c][:2, :2] for c in range(chains)] for base in (low, high)]
        pick = [jnp.where(out_col == 0, v[0], v[1]) for v in values]
        ref[...] = jnp.where(out_row == 0, pick[0], pick[1])

    def drain(k, carry):
        bulk(k).wait_send()
        return carry

    show(HYQ, HYE, hyper_out)
    lax.fori_loop(0, STEPS, drain, 0)
    kick_hyper(STEPS, 0.5)
    show(VEQ, VEE, velocity_out)
    drain(STEPS, 0)


def hand_out(*refs):
    count = (len(refs) - 1) // 2
    sems = refs[-1]
    copies = [pltpu.make_async_copy(refs[i], refs[count + i], sems.at[i]) for i in range(count)]
    for copy in copies:
        copy.start()
    for copy in copies:
        copy.wait()


def solution(mesh):
    nr, nc = mesh.shape["row"], mesh.shape["col"]
    devices = nr * nc

    def shards(latent, momentum, hyper_params, velocity, step_size, counts, kappa_field):
        chains, rows, cols = latent.shape
        tiles = cols // LANES
        deep = rows + 2 * TOP
        total = float(rows * nr * cols * nc)
        sizes = (nr, nc, chains, rows, tiles, total)
        anywhere = pl.BlockSpec(memory_space=pltpu.HBM)
        small = pl.BlockSpec(memory_space=pltpu.VMEM)
        arrays = 2 * chains + 2
        f32 = jnp.float32
        fold_one, fold_two = LANES // (SEG * chains), LANES // (SEG * (chains + 2))
        everywhere = pltpu.VMEM((chains, tiles + 1, deep, LANES), f32)
        inner = pltpu.VMEM((chains, tiles, rows, LANES), f32)
        strip_one = pltpu.VMEM((2, rows // fold_one, LANES), f32)
        strip_two = pltpu.VMEM((2, rows // fold_two, LANES), f32)
        corner = pltpu.VMEM((2, 2, HALO, LANES), f32)
        results = pl.pallas_call(
            functools.partial(kernel, sizes),
            out_shape=(
                jax.ShapeDtypeStruct(latent.shape, f32),
                jax.ShapeDtypeStruct(latent.shape, f32),
                jax.ShapeDtypeStruct(hyper_params.shape, f32),
                jax.ShapeDtypeStruct(velocity.shape, f32),
            ),
            in_specs=[anywhere] * 7,
            out_specs=(small,) * 4,
            scratch_shapes=[
                pltpu.VMEM((arrays, tiles + 1, deep, LANES), f32),
                everywhere,
                pltpu.VMEM((tiles + 1, deep, LANES), f32),
                everywhere,
                everywhere,
                everywhere,
                inner,
                inner,
                pltpu.VMEM((tiles, rows, LANES), jnp.int32),
                everywhere,
                pltpu.VMEM((tiles, rows, LANES), f32),
                strip_one, strip_two, strip_one, strip_two, corner, corner,
                pltpu.VMEM((STEPS + 1, 1, LANES), f32),
                pltpu.VMEM((STEPS + 1, devices, 1, LANES), f32),
                pltpu.VMEM(((6 + COEFS) * chains + 1, 8, LANES), f32),
                pltpu.SMEM(hyper_params.shape, f32),
                pltpu.SMEM(velocity.shape, f32),
                pltpu.SMEM(step_size.shape, f32),
                pltpu.SemaphoreType.DMA((2 * tiles * (chains + 1) + 3,)),
                pltpu.SemaphoreType.DMA((16,)),
                pltpu.SemaphoreType.DMA((16,)),
                pltpu.SemaphoreType.DMA((STEPS + 1,)),
                pltpu.SemaphoreType.DMA((STEPS + 1,)),
                pltpu.SemaphoreType.REGULAR((len(signal_rounds(nr)),)),
            ],
            compiler_params=pltpu.CompilerParams(
                collective_id=0, has_side_effects=True, vmem_limit_bytes=24 * 1024 * 1024
            ),
        )(*(pltpu.with_memory_space_constraint(x, pltpu.HBM) for x in (
            latent, momentum, counts, kappa_field, hyper_params, velocity, step_size
        )))
        return pl.pallas_call(
            hand_out,
            out_shape=[jax.ShapeDtypeStruct(x.shape, f32) for x in results],
            in_specs=[small] * 4,
            out_specs=[pl.BlockSpec(memory_space=pl.ANY)] * 4,
            scratch_shapes=[pltpu.SemaphoreType.DMA((4,))],
            compiler_params=pltpu.CompilerParams(vmem_limit_bytes=8 * 1024 * 1024),
        )(*results)

    placed = (
        P(None, "row", "col"),
        P(None, "row", "col"),
        P(),
        P(),
        P(),
        P("row", "col"),
        P("row", "col"),
    )
    return jax.shard_map(
        shards,
        mesh=mesh,
        in_specs=placed,
        out_specs=(P(None, "row", "col"), P(None, "row", "col"), P(), P()),
        check_vma=False,
    )
```

```python
import functools

import jax
import jax.numpy as jnp
from jax import lax
from jax.experimental import pallas as pl
from jax.experimental.pallas import tpu as pltpu
from jax.sharding import PartitionSpec as P

STEPS = 10
HALO = 16
EDGE = 8
NEEDED = STEPS + 1
PAD = 8
TOP = PAD + HALO
LANES = 128
SEG = 16
MESH, LOGICAL = pl.DeviceIdType.MESH, pl.DeviceIdType.LOGICAL
COEFS = 6


def signal_rounds(nr):
    rounds, reach = [], 1
    while reach < nr // 2:
        rounds.append(reach)
        reach *= 2
    return rounds


def kernel(
    sizes, latent, momentum, counts, kappa, hyper_in, velocity_in, step_in,
    latent_out, momentum_out, hyper_out, velocity_out,
    state, field_u, diagonal, applied, intensity, scaled, scaled_applied, fresh, raw_counts,
    padded, half, pack_one, pack_two, take_one, take_two, corner_out, corner_in,
    payload, gathered, scal, hyper, velocity, step_size,
    load_sem, halo_send, halo_recv, sum_send, sum_recv, round_sem,
):
    nr, nc, chains, rows, tiles, total = sizes
    devices = nr * nc
    row, col = lax.axis_index("row"), lax.axis_index("col")
    me = row * nc + col
    kap, cnt = 2 * chains, 2 * chains + 1
    fold_one, fold_two = LANES // (SEG * chains), LANES // (SEG * (chains + 2))
    rows_one, rows_two = rows // fold_one, rows // fold_two
    own = pl.ds(TOP, rows)
    everything = range(tiles + 1)

    vs, flat = pl.ds(0, chains), pl.ds(0, tiles)
    groups = [[], [], []]
    for j in range(tiles):
        cols = pl.ds(j * LANES, LANES)
        for c in range(chains):
            groups[0].append((latent.at[c, :, cols], state.at[c, j, own, :]))
            groups[1].append((momentum.at[c, :, cols], state.at[chains + c, j, own, :]))
        groups[1].append((kappa.at[:, cols], state.at[kap, j, own, :]))
        groups[2].append((counts.at[:, cols], raw_counts.at[j]))
    groups += [[(hyper_in, hyper)], [(velocity_in, velocity)], [(step_in, step_size)]]
    for i, group in enumerate(groups):
        for source, target in group:
            pltpu.make_async_copy(source, target, load_sem.at[i]).start()
    targets = [state.at[vs, flat, own, :], state.at[pl.ds(chains, chains + 1), flat, own, :], raw_counts]
    targets += [hyper, velocity, step_size]
    loads = [pltpu.make_async_copy(target, target, load_sem.at[i]) for i, target in enumerate(targets)]
    first_loads = 1

    def wrap(d):
        other = me + d % devices
        return jnp.where(other < devices, other, other - devices)

    def flip(x, mask):
        bits = [b for b in (1 << i for i in range(mask.bit_length())) if mask & b]
        return x + sum(b - 2 * b * (x // b % 2) for b in bits)

    def at(dr, dc):
        return (lax.rem(row + (dr + nr), nr), lax.rem(col + (dc + nc), nc))

    barrier = pltpu.get_barrier_semaphore()
    near = [lax.rem(row + r, nr) * nc + c for r in (1, nr - 1) for c in range(nc)]
    near += [row * nc + jnp.where(col + c < nc, col + c, col + c - nc) for c in range(1, nc)]
    for other in near:
        pl.semaphore_signal(barrier, inc=1, device_id=other, device_id_type=LOGICAL)
    if nr & (nr - 1) or nc & (nc - 1):
        others = [wrap(d) for d in range(1, devices)]
    else:
        pairs = [(r, c) for r in range(nr) for c in range(nc) if r or c]
        pairs.sort(key=lambda p: (p[1] & 1) - 2 * (p[0] + bin(p[1] >> 1).count("1")))
        others = [flip(row, r) * nc + flip(col, c) for r, c in pairs]

    lane = lax.broadcasted_iota(jnp.int32, (8, LANES), 1)
    sublane = lax.broadcasted_iota(jnp.int32, (8, LANES), 0)
    lane_row = lax.broadcasted_iota(jnp.int32, (1, LANES), 1)
    seg = lane_row // SEG
    first, last = lane_row == 0, lane_row == LANES - 1

    def fold(x):
        return sum(x[8 * i : 8 * i + 8] for i in range(x.shape[0] // 8))

    def whole(x):
        return jnp.broadcast_to(jnp.sum(jnp.sum(x, axis=0, keepdims=True), axis=1, keepdims=True), (8, LANES))

    def pack(ref, arrays, depth, folds):
        heads = tails = None
        for s in range(folds):
            part = pl.ds(TOP + s * depth, depth)
            for i, a in enumerate(arrays):
                slot = s * len(arrays) + i
                head, tail = state[a, 0, part, :], state[a, tiles - 1, part, :]
                if slot:
                    head = pltpu.roll(head, slot * SEG, 1)
                tail = pltpu.roll(tail, (slot + 1) * SEG % LANES, 1) if (slot + 1) * SEG % LANES else tail
                heads = head if heads is None else jnp.where(seg == slot, head, heads)
                tails = tail if tails is None else jnp.where(seg == slot, tail, tails)
        ref[0] = heads
        ref[1] = tails

    def unpack(right, left, slot_right, slot_left):
        turn = (LANES - SEG * slot_right) % LANES
        right = pltpu.roll(right, turn, 1) if turn else right
        turn = (LANES - SEG - SEG * slot_left) % LANES
        left = pltpu.roll(left, turn, 1) if turn else left
        return jnp.where(seg == 0, right, jnp.where(seg == LANES // SEG - 1, left, 0.0))

    for copy in loads[:first_loads]:
        copy.wait()
    pack(pack_one, list(range(chains)), rows_one, fold_one)
    pl.semaphore_wait(barrier, len(near))

    remotes = []

    def remote(src, dst, where):
        copy = pltpu.make_async_remote_copy(
            src_ref=src, dst_ref=dst, send_sem=halo_send.at[len(remotes)], recv_sem=halo_recv.at[len(remotes)],
            device_id=where, device_id_type=MESH,
        )
        remotes.append(copy)
        copy.start()


    def rowcopies(arrays, near_row, depth):
        remote(
            state.at[arrays, flat, pl.ds(TOP + near_row, depth), :],
            state.at[arrays, flat, pl.ds(TOP + rows + near_row, depth), :],
            at(-1, 0),
        )
        remote(
            state.at[arrays, flat, pl.ds(TOP + rows - near_row - depth, depth), :],
            state.at[arrays, flat, pl.ds(TOP - near_row - depth, depth), :],
            at(1, 0),
        )

    remote(pack_one.at[0], take_one.at[0], at(0, -1))
    remote(pack_one.at[1], take_one.at[1], at(0, 1))
    rowcopies(vs, 0, EDGE)
    stage_one = len(remotes)

    rounds = signal_rounds(nr)

    def tell(i):
        for r in (rounds[i], -rounds[i]):
            pl.semaphore_signal(round_sem.at[i], inc=1, device_id=at(r, 0), device_id_type=MESH)

    tell(0)

    for copy in loads[first_loads:]:
        copy.wait()
    counted = jnp.zeros((8, LANES), jnp.float32)
    for j in range(tiles):
        value = raw_counts[j].astype(jnp.float32)
        state[cnt, j, own, :] = value
        counted += fold(value)
    for vert, start in ((1, TOP), (0, TOP + rows - HALO)):
        heads = tails = None
        for a in range(2 * chains + 2):
            head = state[a, 0, pl.ds(start, HALO), :]
            tail = pltpu.roll(state[a, tiles - 1, pl.ds(start, HALO), :], (a + 1) * SEG % LANES, 1)
            if a:
                head = pltpu.roll(head, a * SEG, 1)
            heads = head if heads is None else jnp.where(seg == a, head, heads)
            tails = tail if tails is None else jnp.where(seg == a, tail, tails)
        corner_out[0, vert] = heads
        corner_out[1, vert] = tails
    rest = pl.ds(chains, chains + 2)
    rowcopies(rest, 0, 1)
    for side, dc in ((0, -1), (1, 1)):
        for vert, dr in ((1, -1), (0, 1)):
            part = pl.ds(0 if vert else HALO - NEEDED, NEEDED)
            remote(corner_out.at[side, vert, part], corner_in.at[side, vert, part], at(dr, dc))
    early = remotes[stage_one:]
    rowcopies(rest, 1, NEEDED - 2)
    rowcopies(vs, EDGE, NEEDED - EDGE)
    bulk_rows = remotes[stage_one + len(early) :]
    pack(pack_two, list(range(chains, 2 * chains + 2)), rows_two, fold_two)
    remote(pack_two.at[0], take_two.at[0], at(0, -1))
    remote(pack_two.at[1], take_two.at[1], at(0, 1))
    early += remotes[-2:]

    h = [step_size[c] for c in range(chains)]
    hh = [h[c] * h[c] for c in range(chains)]

    def full(value):
        return jnp.full((8, LANES), value, jnp.float32)

    TAU, EXO, HYQ, HYE, VEQ, VEE = (i * chains for i in range(6))
    CO = 6 * chains
    LOCAL = CO + COEFS * chains
    for c in range(chains):
        scal[HYQ + c] = full(hyper[1, c])
        scal[HYE + c] = full(hyper[0, c])
        scal[VEQ + c] = full(velocity[1, c])
        scal[VEE + c] = full(velocity[0, c])
        scal[TAU + c] = jnp.exp(full(hyper[1, c]))
        scal[EXO + c] = jnp.exp(full(hyper[0, c]))
    scal[LOCAL] = whole(counted)

    mass = []
    for c in range(chains):
        acc = None
        for j in range(tiles):
            value = jnp.exp(state[c, j, own, :])
            intensity[c, j, own, :] = value
            acc = fold(value) if acc is None else acc + fold(value)
        mass.append(whole(acc))
    for j in range(tiles):
        diag = state[kap, j, own, :] + 4.0
        diagonal[j, own, :] = diag
        half[j] = 0.5 * diag
        for c in range(chains):
            hc = hh[c] * state[cnt, j, own, :]
            scaled[c, j, own, :] = hc
            field_u[c, j, own, :] = state[c, j, own, :] + (h[c] * state[chains + c, j, own, :] + 0.5 * hc)

    def stencil(ref, c, r, deep, lane_tiles):
        rowset = pl.ds(r, deep)
        at_tile = [ref[c, j, rowset, :] for j in everything]
        n = tiles + 1
        used = sorted({(j + s) % n for j in lane_tiles for s in (-1, 0)})
        to_right = {j: pltpu.roll(at_tile[j], 1, 1) for j in used}
        used = sorted({(j + s) % n for j in lane_tiles for s in (1, 0)})
        to_left = {j: pltpu.roll(at_tile[j], LANES - 1, 1) for j in used}
        out = []
        for j in lane_tiles:
            beside = jnp.where(first, to_right[(j - 1) % n], to_right[j])
            beside += jnp.where(last, to_left[(j + 1) % n], to_left[j])
            beside += ref[c, j, pl.ds(r - 1, deep), :] + ref[c, j, pl.ds(r + 1, deep), :]
            out.append((j, at_tile[j], diagonal[j, rowset, :] * at_tile[j] - beside))
        return out

    def half_stencil(ref, c, r, deep):
        rowset = pl.ds(r, deep)
        at_tile = [ref[c, j, rowset, :] for j in everything]
        to_left = [pltpu.roll(x, LANES - 1, 1) for x in at_tile]
        out = []
        for j in range(tiles):
            beside = jnp.where(last, to_left[j + 1], to_left[j]) + ref[c, j, pl.ds(r + 1, deep), :]
            out.append((j, at_tile[j], half[j, pl.ds(r - TOP, deep), :] * at_tile[j] - beside))
        return out

    DEEP = 64

    def own_blocks():
        return [TOP + i * DEEP for i in range(rows // DEEP)]

    def flanks():
        return [(r, DEEP, [tiles]) for r in own_blocks()]

    def ends():
        return [(PAD, HALO, everything), (TOP + rows, HALO, everything)]

    def sides():
        return flanks() + ends()

    def own_applied(ref):
        quads = []
        for c in range(chains):
            acc = jnp.zeros((8, LANES), jnp.float32)
            for r in own_blocks():
                for j, v, av in stencil(ref, c, r, DEEP, range(tiles)):
                    applied[c, j, pl.ds(r, DEEP), :] = av
                    acc += fold(v * av)
            quads.append(acc)
        return quads

    def halo_applied(regions):
        for c in range(chains):
            for r, deep, lane_tiles in regions:
                for j, _, av in stencil(state, c, r, deep, lane_tiles):
                    applied[c, j, pl.ds(r, deep), :] = av

    def send(k, quad, mass):
        out = scal[LOCAL][:1]
        for i, value in enumerate(quad + mass):
            out = jnp.where(seg == i, value[:1], out)
        payload[k] = out
        gathered[k, pl.ds(me, 1), :] = out
        for other in others:
            pltpu.make_async_remote_copy(
                src_ref=payload.at[k], dst_ref=gathered.at[k, pl.ds(me, 1), :],
                send_sem=sum_send, recv_sem=sum_recv.at[k],
                device_id=other, device_id_type=LOGICAL,
            ).start()

    def bulk(k):
        ref = gathered.at[k, pl.ds(0, devices - 1), :]
        return pltpu.make_async_remote_copy(
            src_ref=ref, dst_ref=ref, send_sem=sum_send, recv_sem=sum_recv.at[0 if isinstance(k, pl.Slice) else k],
            device_id=others[0], device_id_type=LOGICAL,
        )

    def collect(k):
        bulk(k).wait_recv()
        summed = jnp.broadcast_to(jnp.sum(gathered[k], axis=0, keepdims=True), (8, LANES))
        values = [
            jnp.broadcast_to(jnp.sum(jnp.where(lane == i * SEG, summed, 0.0), axis=1, keepdims=True), (8, LANES))
            for i in range(2 * chains + 1)
        ]
        return values[:chains], values[chains : 2 * chains], values[2 * chains]

    def kick_hyper(k, part):
        quad, mass, number = collect(k)
        for c in range(chains):
            aq = (0.5 / total) * (scal[TAU + c] * quad[c]) - 0.5
            ae = (scal[EXO + c] * mass[c] - number) * (1.0 / total)
            scal[VEQ + c] = scal[VEQ + c] - (part * h[c]) * aq
            scal[VEE + c] = scal[VEE + c] - (part * h[c]) * ae

    def drift_hyper():
        for c in range(chains):
            q = scal[HYQ + c] + h[c] * scal[VEQ + c]
            e = scal[HYE + c] + h[c] * scal[VEE + c]
            scal[HYQ + c] = q
            scal[HYE + c] = e
            scal[TAU + c] = jnp.exp(q)
            scal[EXO + c] = jnp.exp(e)

    def weights(part):
        xs = [(part * hh[c]) * scal[TAU + c] for c in range(chains)]
        ys = [(part * hh[c]) * scal[EXO + c] for c in range(chains)]
        return xs, ys

    def own_fresh(xs, ys):
        out = []
        for c in range(chains):
            x, y = xs[c][:1], ys[c][:1]
            acc = jnp.zeros((8, LANES), jnp.float32)
            for j in range(tiles):
                v = field_u[c, j, own, :] - x * applied[c, j, own, :] - y * intensity[c, j, own, :]
                value = jnp.exp(v)
                fresh[c, j] = v
                intensity[c, j, own, :] = value
                acc += fold(value)
            out.append(acc)
        return [whole(acc) for acc in out]

    def own_settle():
        for c in range(chains):
            for j in range(tiles):
                v = fresh[c, j]
                field_u[c, j, own, :] = (v + v) - state[c, j, own, :] + scaled[c, j, own, :]
                state[c, j, own, :] = v

    def halo_advance(xs, ys):
        for c in range(chains):
            x, y = xs[c][:1], ys[c][:1]
            for r, deep, lane_tiles in sides():
                rowset = pl.ds(r, deep)
                for j in lane_tiles:
                    v = field_u[c, j, rowset, :] - x * applied[c, j, rowset, :] - y * intensity[c, j, rowset, :]
                    field_u[c, j, rowset, :] = (v + v) - state[c, j, rowset, :] + scaled[c, j, rowset, :]
                    intensity[c, j, rowset, :] = jnp.exp(v)
                    state[c, j, rowset, :] = v

    def own_coefs(direct):
        for c in range(chains):
            sums = [jnp.zeros((8, LANES), jnp.float32)] * COEFS
            if not direct:
                for r in own_blocks():
                    rowset = pl.ds(r, DEEP)
                    for j, v, av in stencil(state, c, r, DEEP, range(tiles)):
                        au = (av + av) - applied[c, j, rowset, :] + scaled_applied[c, j, pl.ds(r - TOP, DEEP), :]
                        applied[c, j, rowset, :] = av
                        sums[0] += fold(field_u[c, j, rowset, :] * au)
                        sums[1] += fold(av * au)
                        sums[2] += fold(intensity[c, j, rowset, :] * au)
            yield c, sums

    def finish_coefs(direct, c, sums):
        for r in own_blocks():
            rowset = pl.ds(r, DEEP)
            if direct:
                for j, u, au in stencil(field_u, c, r, DEEP, range(tiles)):
                    sums[0] += fold(u * au)
                    sums[1] += fold(applied[c, j, rowset, :] * au)
                    sums[2] += fold(intensity[c, j, rowset, :] * au)
            for (j, a, ta), (_, e, te) in zip(half_stencil(applied, c, r, DEEP), half_stencil(intensity, c, r, DEEP)):
                sums[3] += fold(a * ta)
                sums[4] += fold(e * ta + a * te)
                sums[5] += fold(e * te)
        for i in range(COEFS):
            total_i = whole(sums[i])
            scal[CO + COEFS * c + i] = total_i + total_i if i in (3, 5) else total_i

    def predicted(xs, ys):
        out = []
        for c in range(chains):
            k0, k1, k2, k3, k4, k5 = [scal[CO + COEFS * c + i] for i in range(COEFS)]
            x, y = xs[c], ys[c]
            out.append(k0 - 2.0 * (x * k1 + y * k2) + (x * (x * k3 + 2.0 * (y * k4)) + y * (y * k5)))
        return out

    for c in range(chains):
        for r in (TOP - 8, TOP + rows):
            for j in range(tiles):
                padded[c, j, pl.ds(r, 8), :] = jnp.zeros((8, LANES), jnp.float32)
        padded[c, tiles, own, :] = jnp.zeros((rows, LANES), jnp.float32)
        for j in range(tiles):
            padded[c, j, own, :] = state[c, j, own, :]
    quad = own_applied(padded)
    place = lane_row % SEG

    for i in range(len(rounds)):
        pl.semaphore_wait(round_sem.at[i], 2)
        if i + 1 < len(rounds):
            tell(i + 1)
    for copy in remotes[:stage_one]:
        copy.wait_recv()
    across = jnp.where(place == SEG - 1, pack_one[1] * pltpu.roll(take_one[0], SEG - 1, 1), 0.0)
    across += jnp.where(place == 0, pack_one[0] * pltpu.roll(take_one[1], LANES - SEG + 1, 1), 0.0)
    across = fold(across)
    for c in range(chains):
        along = sum(
            state[c, j, pl.ds(TOP, 1), :] * state[c, j, pl.ds(TOP - 1, 1), :]
            + state[c, j, pl.ds(TOP + rows - 1, 1), :] * state[c, j, pl.ds(TOP + rows, 1), :]
            for j in range(tiles)
        )
        quad[c] = whole(quad[c] - jnp.where(seg % chains == c, across, 0.0) - jnp.where(sublane == 0, along, 0.0))
    send(0, quad, mass)

    for c in range(chains):
        for s in range(fold_one):
            slot = s * chains + c
            part = pl.ds(TOP + s * rows_one, rows_one)
            side = unpack(take_one[0], take_one[1], slot, slot)
            state[c, tiles, part, :] = side
            applied[c, 0, part, :] = applied[c, 0, part, :] - jnp.where(first, pltpu.roll(side, 1, 1), 0.0)
            applied[c, tiles - 1, part, :] = applied[c, tiles - 1, part, :] - jnp.where(
                last, pltpu.roll(side, LANES - 1, 1), 0.0
            )
        for j in range(tiles):
            for here, there in ((TOP, TOP - 1), (TOP + rows - 1, TOP + rows)):
                here, there = pl.ds(here, 1), pl.ds(there, 1)
                applied[c, j, here, :] = applied[c, j, here, :] - state[c, j, there, :]

    xs, ys = weights(0.5)
    mass = own_fresh(xs, ys)

    for copy in early:
        copy.wait_recv()
    for s in range(fold_two):
        for i in range(chains + 2):
            slot = s * (chains + 2) + i
            state[chains + i, tiles, pl.ds(TOP + s * rows_two, rows_two), :] = unpack(
                take_two[0], take_two[1], slot, slot
            )
    for vert, r in ((0, PAD), (1, TOP + rows)):
        for a in range(2 * chains + 2):
            state[a, tiles, pl.ds(r, HALO), :] = unpack(corner_in[0, vert], corner_in[1, vert], a, a)
    def halo_start(regions):
        for r, deep, lane_tiles in regions:
            rowset = pl.ds(r, deep)
            for j in lane_tiles:
                diagonal[j, rowset, :] = state[kap, j, rowset, :] + 4.0
                for c in range(chains):
                    hc = hh[c] * state[cnt, j, rowset, :]
                    scaled[c, j, rowset, :] = hc
                    v = state[c, j, rowset, :]
                    intensity[c, j, rowset, :] = jnp.exp(v)
                    field_u[c, j, rowset, :] = v + (h[c] * state[chains + c, j, rowset, :] + 0.5 * hc)

    halo_start(flanks())
    halo_applied(flanks())
    for c in range(chains):
        x, y = xs[c][:1], ys[c][:1]
        padded[c, tiles, own, :] = (
            field_u[c, tiles, own, :] - x * applied[c, tiles, own, :] - y * intensity[c, tiles, own, :]
        )
        for r in (TOP - 1, TOP + rows):
            line = pl.ds(r, 1)
            cells = [state[c, j, line, :] for j in everything]
            to_right, to_left = [pltpu.roll(z, 1, 1) for z in cells], [pltpu.roll(z, LANES - 1, 1) for z in cells]
            for j in range(tiles):
                beside = jnp.where(first, to_right[(j - 1) % (tiles + 1)], to_right[j])
                beside += jnp.where(last, to_left[j + 1], to_left[j])
                beside += state[c, j, pl.ds(r - 1, 1), :] + state[c, j, pl.ds(r + 1, 1), :]
                av = (state[kap, j, line, :] + 4.0) * cells[j] - beside
                u = cells[j] + (h[c] * state[chains + c, j, line, :] + 0.5 * (hh[c] * state[cnt, j, line, :]))
                padded[c, j, line, :] = u - x * av - y * jnp.exp(cells[j])
        for j in range(tiles):
            padded[c, j, own, :] = fresh[c, j]
    send(1, [whole(q) for q in own_applied(padded)], mass)

    for copy in bulk_rows:
        copy.wait_recv()
    for copy in remotes:
        copy.wait_send()
    halo_start(ends())
    halo_applied(ends())
    halo_advance(xs, ys)
    own_settle()
    halo_applied(sides())
    for r in own_blocks():
        for j, _, value in stencil(state, cnt, r, DEEP, range(tiles)):
            for c in range(chains):
                scaled_applied[c, j, pl.ds(r - TOP, DEEP), :] = hh[c] * value
    for c, sums in own_coefs(True):
        finish_coefs(True, c, sums)

    def step(k, carry):
        kick_hyper(k - 1, jnp.where(k == 1, 0.5, 1.0))
        drift_hyper()
        xs, ys = weights(1.0)
        mass = own_fresh(xs, ys)
        send(k + 1, predicted(xs, ys), mass)
        halo_advance(xs, ys)
        own_settle()
        pairs = list(own_coefs(False))
        halo_applied(sides())
        for c, sums in pairs:
            finish_coefs(False, c, sums)
        return carry

    lax.fori_loop(1, STEPS, step, 0)

    for c in range(chains):
        for j in range(tiles):
            latent_out[c, :, pl.ds(j * LANES, LANES)] = state[c, j, own, :]
    kick_hyper(STEPS - 1, 1.0)
    drift_hyper()
    xs, ys = weights(0.5)
    for c in range(chains):
        x, y = xs[c][:1], ys[c][:1]
        for j in range(tiles):
            moved = field_u[c, j, own, :] - state[c, j, own, :] - 0.5 * scaled[c, j, own, :]
            moved = moved - x * applied[c, j, own, :] - y * intensity[c, j, own, :]
            momentum_out[c, :, pl.ds(j * LANES, LANES)] = moved * (1.0 / full(h[c])[:1])
    out_row, out_col = sublane[:2, :2], lane[:2, :2]

    def show(high, low, ref):
        values = [[scal[base + c][:2, :2] for c in range(chains)] for base in (low, high)]
        pick = [jnp.where(out_col == 0, v[0], v[1]) for v in values]
        ref[...] = jnp.where(out_row == 0, pick[0], pick[1])

    show(HYQ, HYE, hyper_out)
    kick_hyper(STEPS, 0.5)
    show(VEQ, VEE, velocity_out)
    bulk(pl.ds(0, STEPS + 1)).wait_send()


def hand_out(*refs):
    count = (len(refs) - 1) // 2
    sems = refs[-1]
    copies = [pltpu.make_async_copy(refs[i], refs[count + i], sems.at[i]) for i in range(count)]
    for copy in copies:
        copy.start()
    for copy in copies:
        copy.wait()


def solution(mesh):
    nr, nc = mesh.shape["row"], mesh.shape["col"]
    devices = nr * nc

    def shards(latent, momentum, hyper_params, velocity, step_size, counts, kappa_field):
        chains, rows, cols = latent.shape
        tiles = cols // LANES
        deep = rows + 2 * TOP
        total = float(rows * nr * cols * nc)
        sizes = (nr, nc, chains, rows, tiles, total)
        anywhere = pl.BlockSpec(memory_space=pltpu.HBM)
        small = pl.BlockSpec(memory_space=pltpu.VMEM)
        arrays = 2 * chains + 2
        f32 = jnp.float32
        fold_one, fold_two = LANES // (SEG * chains), LANES // (SEG * (chains + 2))
        everywhere = pltpu.VMEM((chains, tiles + 1, deep, LANES), f32)
        inner = pltpu.VMEM((chains, tiles, rows, LANES), f32)
        strip_one = pltpu.VMEM((2, rows // fold_one, LANES), f32)
        strip_two = pltpu.VMEM((2, rows // fold_two, LANES), f32)
        corner = pltpu.VMEM((2, 2, HALO, LANES), f32)
        results = pl.pallas_call(
            functools.partial(kernel, sizes),
            out_shape=(
                jax.ShapeDtypeStruct(latent.shape, f32),
                jax.ShapeDtypeStruct(latent.shape, f32),
                jax.ShapeDtypeStruct(hyper_params.shape, f32),
                jax.ShapeDtypeStruct(velocity.shape, f32),
            ),
            in_specs=[anywhere] * 7,
            out_specs=(small,) * 4,
            scratch_shapes=[
                pltpu.VMEM((arrays, tiles + 1, deep, LANES), f32),
                everywhere,
                pltpu.VMEM((tiles + 1, deep, LANES), f32),
                everywhere,
                everywhere,
                everywhere,
                inner,
                inner,
                pltpu.VMEM((tiles, rows, LANES), jnp.int32),
                everywhere,
                pltpu.VMEM((tiles, rows, LANES), f32),
                strip_one, strip_two, strip_one, strip_two, corner, corner,
                pltpu.VMEM((STEPS + 1, 1, LANES), f32),
                pltpu.VMEM((STEPS + 1, devices, LANES), f32),
                pltpu.VMEM(((6 + COEFS) * chains + 1, 8, LANES), f32),
                pltpu.SMEM(hyper_params.shape, f32),
                pltpu.SMEM(velocity.shape, f32),
                pltpu.SMEM(step_size.shape, f32),
                pltpu.SemaphoreType.DMA((6,)),
                pltpu.SemaphoreType.DMA((16,)),
                pltpu.SemaphoreType.DMA((16,)),
                pltpu.SemaphoreType.DMA,
                pltpu.SemaphoreType.DMA((STEPS + 1,)),
                pltpu.SemaphoreType.REGULAR((len(signal_rounds(nr)),)),
            ],
            compiler_params=pltpu.CompilerParams(
                collective_id=0, has_side_effects=True, vmem_limit_bytes=24 * 1024 * 1024
            ),
        )(*(pltpu.with_memory_space_constraint(x, pltpu.HBM) for x in (
            latent, momentum, counts, kappa_field, hyper_params, velocity, step_size
        )))
        return pl.pallas_call(
            hand_out,
            out_shape=[jax.ShapeDtypeStruct(x.shape, f32) for x in results],
            in_specs=[small] * 4,
            out_specs=[pl.BlockSpec(memory_space=pl.ANY)] * 4,
            scratch_shapes=[pltpu.SemaphoreType.DMA((4,))],
            compiler_params=pltpu.CompilerParams(vmem_limit_bytes=8 * 1024 * 1024),
        )(*results)

    placed = (
        P(None, "row", "col"),
        P(None, "row", "col"),
        P(),
        P(),
        P(),
        P("row", "col"),
        P("row", "col"),
    )
    return jax.shard_map(
        shards,
        mesh=mesh,
        in_specs=placed,
        out_specs=(P(None, "row", "col"), P(None, "row", "col"), P(), P()),
        check_vma=False,
    )
```

```python
import functools

import jax
import jax.numpy as jnp
from jax import lax
from jax.experimental import pallas as pl
from jax.experimental.pallas import tpu as pltpu
from jax.sharding import PartitionSpec as P

STEPS = 10
HALO = 16
EDGE = 8
NEEDED = STEPS + 1
PAD = 8
TOP = PAD + HALO
LANES = 128
SEG = 16
MESH, LOGICAL = pl.DeviceIdType.MESH, pl.DeviceIdType.LOGICAL
COEFS = 6


def signal_rounds(nr):
    rounds, reach = [], 1
    while reach < nr // 2:
        rounds.append(reach)
        reach *= 2
    return rounds


def kernel(
    sizes, latent, momentum, counts, kappa, hyper_in, velocity_in, step_in,
    latent_out, momentum_out, hyper_out, velocity_out,
    state, field_u, diagonal, applied, intensity, scaled, scaled_applied, fresh, raw_counts,
    padded, half, pack_one, pack_two, take_one, take_two, corner_out, corner_in,
    payload, gathered, scal, hyper, velocity, step_size,
    load_sem, halo_send, halo_recv, sum_send, sum_recv, round_sem,
):
    nr, nc, chains, rows, tiles, total = sizes
    devices = nr * nc
    row, col = lax.axis_index("row"), lax.axis_index("col")
    me = row * nc + col
    kap, cnt = 2 * chains, 2 * chains + 1
    fold_one, fold_two = LANES // (SEG * chains), LANES // (SEG * (chains + 2))
    rows_one, rows_two = rows // fold_one, rows // fold_two
    own = pl.ds(TOP, rows)
    everything = range(tiles + 1)

    vs, flat = pl.ds(0, chains), pl.ds(0, tiles)
    groups = [[], [], []]
    for j in range(tiles):
        cols = pl.ds(j * LANES, LANES)
        for c in range(chains):
            groups[0].append((latent.at[c, :, cols], state.at[c, j, own, :]))
            groups[1].append((momentum.at[c, :, cols], state.at[chains + c, j, own, :]))
        groups[1].append((kappa.at[:, cols], state.at[kap, j, own, :]))
        groups[2].append((counts.at[:, cols], raw_counts.at[j]))
    groups += [[(hyper_in, hyper)], [(velocity_in, velocity)], [(step_in, step_size)]]
    for i, group in enumerate(groups):
        for source, target in group:
            pltpu.make_async_copy(source, target, load_sem.at[i]).start()
    targets = [state.at[vs, flat, own, :], state.at[pl.ds(chains, chains + 1), flat, own, :], raw_counts]
    targets += [hyper, velocity, step_size]
    loads = [pltpu.make_async_copy(target, target, load_sem.at[i]) for i, target in enumerate(targets)]
    first_loads = 1

    def wrap(d):
        other = me + d % devices
        return jnp.where(other < devices, other, other - devices)

    def flip(x, mask):
        bits = [b for b in (1 << i for i in range(mask.bit_length())) if mask & b]
        return x + sum(b - 2 * b * (x // b % 2) for b in bits)

    def at(dr, dc):
        return (lax.rem(row + (dr + nr), nr), lax.rem(col + (dc + nc), nc))

    barrier = pltpu.get_barrier_semaphore()
    near = [lax.rem(row + r, nr) * nc + c for r in (1, nr - 1) for c in range(nc)]
    near += [row * nc + jnp.where(col + c < nc, col + c, col + c - nc) for c in range(1, nc)]
    for other in near:
        pl.semaphore_signal(barrier, inc=1, device_id=other, device_id_type=LOGICAL)
    if nr & (nr - 1) or nc & (nc - 1):
        others = [wrap(d) for d in range(1, devices)]
    else:
        pairs = [(r, c) for r in range(nr) for c in range(nc) if r or c]
        pairs.sort(key=lambda p: (p[1] & 1) - 2 * (p[0] + bin(p[1] >> 1).count("1")))
        others = [flip(row, r) * nc + flip(col, c) for r, c in pairs]

    lane = lax.broadcasted_iota(jnp.int32, (8, LANES), 1)
    sublane = lax.broadcasted_iota(jnp.int32, (8, LANES), 0)
    lane_row = lax.broadcasted_iota(jnp.int32, (1, LANES), 1)
    seg = lane_row // SEG
    first, last = lane_row == 0, lane_row == LANES - 1

    def fold(x):
        parts = [x[8 * i : 8 * i + 8] for i in range(x.shape[0] // 8)]
        lines = [sum(parts[i::4]) for i in range(4)] if len(parts) > 8 else parts
        return sum(lines)

    def whole(x):
        return jnp.broadcast_to(jnp.sum(jnp.sum(x, axis=0, keepdims=True), axis=1, keepdims=True), (8, LANES))

    def pack(ref, arrays, depth, folds):
        heads = tails = None
        for s in range(folds):
            part = pl.ds(TOP + s * depth, depth)
            for i, a in enumerate(arrays):
                slot = s * len(arrays) + i
                head, tail = state[a, 0, part, :], state[a, tiles - 1, part, :]
                if slot:
                    head = pltpu.roll(head, slot * SEG, 1)
                tail = pltpu.roll(tail, (slot + 1) * SEG % LANES, 1) if (slot + 1) * SEG % LANES else tail
                heads = head if heads is None else jnp.where(seg == slot, head, heads)
                tails = tail if tails is None else jnp.where(seg == slot, tail, tails)
        ref[0] = heads
        ref[1] = tails

    def unpack(right, left, slot_right, slot_left):
        turn = (LANES - SEG * slot_right) % LANES
        right = pltpu.roll(right, turn, 1) if turn else right
        turn = (LANES - SEG - SEG * slot_left) % LANES
        left = pltpu.roll(left, turn, 1) if turn else left
        return jnp.where(seg == 0, right, jnp.where(seg == LANES // SEG - 1, left, 0.0))

    for copy in loads[:first_loads]:
        copy.wait()
    pack(pack_one, list(range(chains)), rows_one, fold_one)
    pl.semaphore_wait(barrier, len(near))

    remotes = []

    def remote(src, dst, where):
        copy = pltpu.make_async_remote_copy(
            src_ref=src, dst_ref=dst, send_sem=halo_send.at[len(remotes)], recv_sem=halo_recv.at[len(remotes)],
            device_id=where, device_id_type=MESH,
        )
        remotes.append(copy)
        copy.start()


    def rowcopies(arrays, near_row, depth):
        remote(
            state.at[arrays, flat, pl.ds(TOP + near_row, depth), :],
            state.at[arrays, flat, pl.ds(TOP + rows + near_row, depth), :],
            at(-1, 0),
        )
        remote(
            state.at[arrays, flat, pl.ds(TOP + rows - near_row - depth, depth), :],
            state.at[arrays, flat, pl.ds(TOP - near_row - depth, depth), :],
            at(1, 0),
        )

    remote(pack_one.at[0], take_one.at[0], at(0, -1))
    remote(pack_one.at[1], take_one.at[1], at(0, 1))
    rowcopies(vs, 0, EDGE)
    stage_one = len(remotes)

    rounds = signal_rounds(nr)

    def tell(i):
        for r in (rounds[i], -rounds[i]):
            pl.semaphore_signal(round_sem.at[i], inc=1, device_id=at(r, 0), device_id_type=MESH)

    tell(0)

    for copy in loads[first_loads:]:
        copy.wait()
    counted = jnp.zeros((8, LANES), jnp.float32)
    for j in range(tiles):
        value = raw_counts[j].astype(jnp.float32)
        state[cnt, j, own, :] = value
        counted += fold(value)
    for vert, start in ((1, TOP), (0, TOP + rows - HALO)):
        heads = tails = None
        for a in range(2 * chains + 2):
            head = state[a, 0, pl.ds(start, HALO), :]
            tail = pltpu.roll(state[a, tiles - 1, pl.ds(start, HALO), :], (a + 1) * SEG % LANES, 1)
            if a:
                head = pltpu.roll(head, a * SEG, 1)
            heads = head if heads is None else jnp.where(seg == a, head, heads)
            tails = tail if tails is None else jnp.where(seg == a, tail, tails)
        corner_out[0, vert] = heads
        corner_out[1, vert] = tails
    rest = pl.ds(chains, chains + 2)
    rowcopies(rest, 0, 1)
    for side, dc in ((0, -1), (1, 1)):
        for vert, dr in ((1, -1), (0, 1)):
            part = pl.ds(0 if vert else HALO - NEEDED, NEEDED)
            remote(corner_out.at[side, vert, part], corner_in.at[side, vert, part], at(dr, dc))
    early = remotes[stage_one:]
    rowcopies(rest, 1, NEEDED - 2)
    rowcopies(vs, EDGE, NEEDED - EDGE)
    bulk_rows = remotes[stage_one + len(early) :]
    pack(pack_two, list(range(chains, 2 * chains + 2)), rows_two, fold_two)
    remote(pack_two.at[0], take_two.at[0], at(0, -1))
    remote(pack_two.at[1], take_two.at[1], at(0, 1))
    early += remotes[-2:]

    h = [step_size[c] for c in range(chains)]
    hh = [h[c] * h[c] for c in range(chains)]

    def full(value):
        return jnp.full((8, LANES), value, jnp.float32)

    TAU, EXO, HYQ, HYE, VEQ, VEE = (i * chains for i in range(6))
    CO = 6 * chains
    LOCAL = CO + COEFS * chains
    for c in range(chains):
        scal[HYQ + c] = full(hyper[1, c])
        scal[HYE + c] = full(hyper[0, c])
        scal[VEQ + c] = full(velocity[1, c])
        scal[VEE + c] = full(velocity[0, c])
        scal[TAU + c] = jnp.exp(full(hyper[1, c]))
        scal[EXO + c] = jnp.exp(full(hyper[0, c]))
    scal[LOCAL] = whole(counted)

    mass = []
    for c in range(chains):
        acc = None
        for j in range(tiles):
            value = jnp.exp(state[c, j, own, :])
            intensity[c, j, own, :] = value
            acc = fold(value) if acc is None else acc + fold(value)
        mass.append(whole(acc))
    for j in range(tiles):
        diag = state[kap, j, own, :] + 4.0
        diagonal[j, own, :] = diag
        half[j] = 0.5 * diag
        for c in range(chains):
            hc = hh[c] * state[cnt, j, own, :]
            scaled[c, j, own, :] = hc
            field_u[c, j, own, :] = state[c, j, own, :] + (h[c] * state[chains + c, j, own, :] + 0.5 * hc)

    def stencil(ref, c, r, deep, lane_tiles):
        rowset = pl.ds(r, deep)
        at_tile = [ref[c, j, rowset, :] for j in everything]
        n = tiles + 1
        used = sorted({(j + s) % n for j in lane_tiles for s in (-1, 0)})
        to_right = {j: pltpu.roll(at_tile[j], 1, 1) for j in used}
        used = sorted({(j + s) % n for j in lane_tiles for s in (1, 0)})
        to_left = {j: pltpu.roll(at_tile[j], LANES - 1, 1) for j in used}
        out = []
        for j in lane_tiles:
            beside = jnp.where(first, to_right[(j - 1) % n], to_right[j])
            beside += jnp.where(last, to_left[(j + 1) % n], to_left[j])
            beside += ref[c, j, pl.ds(r - 1, deep), :] + ref[c, j, pl.ds(r + 1, deep), :]
            out.append((j, at_tile[j], diagonal[j, rowset, :] * at_tile[j] - beside))
        return out

    def half_stencil(ref, c, r, deep):
        rowset = pl.ds(r, deep)
        at_tile = [ref[c, j, rowset, :] for j in everything]
        to_left = [pltpu.roll(x, LANES - 1, 1) for x in at_tile]
        out = []
        for j in range(tiles):
            beside = jnp.where(last, to_left[j + 1], to_left[j]) + ref[c, j, pl.ds(r + 1, deep), :]
            out.append((j, at_tile[j], half[j, pl.ds(r - TOP, deep), :] * at_tile[j] - beside))
        return out

    DEEP = 64

    def own_blocks():
        return [TOP + i * DEEP for i in range(rows // DEEP)]

    def flanks():
        return [(r, DEEP, [tiles]) for r in own_blocks()]

    def ends():
        return [(PAD, HALO, everything), (TOP + rows, HALO, everything)]

    def sides():
        return flanks() + ends()

    def own_applied(ref):
        quads = []
        for c in range(chains):
            acc = jnp.zeros((8, LANES), jnp.float32)
            for r in own_blocks():
                for j, v, av in stencil(ref, c, r, DEEP, range(tiles)):
                    applied[c, j, pl.ds(r, DEEP), :] = av
                    acc += fold(v * av)
            quads.append(acc)
        return quads

    def halo_applied(regions):
        for c in range(chains):
            for r, deep, lane_tiles in regions:
                for j, _, av in stencil(state, c, r, deep, lane_tiles):
                    applied[c, j, pl.ds(r, deep), :] = av

    def send(k, quad, mass):
        out = scal[LOCAL][:1]
        for i, value in enumerate(quad + mass):
            out = jnp.where(seg == i, value[:1], out)
        payload[k] = out
        gathered[k, pl.ds(me, 1), :] = out
        for other in others:
            pltpu.make_async_remote_copy(
                src_ref=payload.at[k], dst_ref=gathered.at[k, pl.ds(me, 1), :],
                send_sem=sum_send, recv_sem=sum_recv.at[k],
                device_id=other, device_id_type=LOGICAL,
            ).start()

    def bulk(k):
        ref = gathered.at[k, pl.ds(0, devices - 1), :]
        return pltpu.make_async_remote_copy(
            src_ref=ref, dst_ref=ref, send_sem=sum_send, recv_sem=sum_recv.at[0 if isinstance(k, pl.Slice) else k],
            device_id=others[0], device_id_type=LOGICAL,
        )

    def collect(k):
        bulk(k).wait_recv()
        summed = jnp.broadcast_to(jnp.sum(gathered[k], axis=0, keepdims=True), (8, LANES))
        values = [
            jnp.broadcast_to(jnp.sum(jnp.where(lane == i * SEG, summed, 0.0), axis=1, keepdims=True), (8, LANES))
            for i in range(2 * chains + 1)
        ]
        return values[:chains], values[chains : 2 * chains], values[2 * chains]

    def kick_hyper(k, part):
        quad, mass, number = collect(k)
        for c in range(chains):
            aq = (0.5 / total) * (scal[TAU + c] * quad[c]) - 0.5
            ae = (scal[EXO + c] * mass[c] - number) * (1.0 / total)
            scal[VEQ + c] = scal[VEQ + c] - (part * h[c]) * aq
            scal[VEE + c] = scal[VEE + c] - (part * h[c]) * ae

    def drift_hyper():
        for c in range(chains):
            q = scal[HYQ + c] + h[c] * scal[VEQ + c]
            e = scal[HYE + c] + h[c] * scal[VEE + c]
            scal[HYQ + c] = q
            scal[HYE + c] = e
            scal[TAU + c] = jnp.exp(q)
            scal[EXO + c] = jnp.exp(e)

    def weights(part):
        xs = [(part * hh[c]) * scal[TAU + c] for c in range(chains)]
        ys = [(part * hh[c]) * scal[EXO + c] for c in range(chains)]
        return xs, ys

    def own_fresh(xs, ys):
        out = []
        for c in range(chains):
            x, y = xs[c][:1], ys[c][:1]
            acc = jnp.zeros((8, LANES), jnp.float32)
            for j in range(tiles):
                v = field_u[c, j, own, :] - x * applied[c, j, own, :] - y * intensity[c, j, own, :]
                value = jnp.exp(v)
                fresh[c, j] = v
                intensity[c, j, own, :] = value
                acc += fold(value)
            out.append(acc)
        return [whole(acc) for acc in out]

    def own_settle():
        for c in range(chains):
            for j in range(tiles):
                v = fresh[c, j]
                field_u[c, j, own, :] = (v + v) - state[c, j, own, :] + scaled[c, j, own, :]
                state[c, j, own, :] = v

    def halo_advance(xs, ys):
        for c in range(chains):
            x, y = xs[c][:1], ys[c][:1]
            for r, deep, lane_tiles in sides():
                rowset = pl.ds(r, deep)
                for j in lane_tiles:
                    v = field_u[c, j, rowset, :] - x * applied[c, j, rowset, :] - y * intensity[c, j, rowset, :]
                    field_u[c, j, rowset, :] = (v + v) - state[c, j, rowset, :] + scaled[c, j, rowset, :]
                    intensity[c, j, rowset, :] = jnp.exp(v)
                    state[c, j, rowset, :] = v

    def own_coefs(direct):
        for c in range(chains):
            sums = [jnp.zeros((8, LANES), jnp.float32)] * COEFS
            if not direct:
                for r in own_blocks():
                    rowset = pl.ds(r, DEEP)
                    for j, v, av in stencil(state, c, r, DEEP, range(tiles)):
                        au = (av + av) - applied[c, j, rowset, :] + scaled_applied[c, j, pl.ds(r - TOP, DEEP), :]
                        applied[c, j, rowset, :] = av
                        sums[0] += fold(field_u[c, j, rowset, :] * au)
                        sums[1] += fold(av * au)
                        sums[2] += fold(intensity[c, j, rowset, :] * au)
            yield c, sums

    def finish_coefs(direct, c, sums):
        for r in own_blocks():
            rowset = pl.ds(r, DEEP)
            if direct:
                for j, u, au in stencil(field_u, c, r, DEEP, range(tiles)):
                    sums[0] += fold(u * au)
                    sums[1] += fold(applied[c, j, rowset, :] * au)
                    sums[2] += fold(intensity[c, j, rowset, :] * au)
            for (j, a, ta), (_, e, te) in zip(half_stencil(applied, c, r, DEEP), half_stencil(intensity, c, r, DEEP)):
                sums[3] += fold(a * ta)
                sums[4] += fold(e * ta + a * te)
                sums[5] += fold(e * te)
        for i in range(COEFS):
            total_i = whole(sums[i])
            scal[CO + COEFS * c + i] = total_i + total_i if i in (3, 5) else total_i

    def predicted(xs, ys):
        out = []
        for c in range(chains):
            k0, k1, k2, k3, k4, k5 = [scal[CO + COEFS * c + i] for i in range(COEFS)]
            x, y = xs[c], ys[c]
            out.append(k0 - 2.0 * (x * k1 + y * k2) + (x * (x * k3 + 2.0 * (y * k4)) + y * (y * k5)))
        return out

    for c in range(chains):
        for r in (TOP - 8, TOP + rows):
            for j in range(tiles):
                padded[c, j, pl.ds(r, 8), :] = jnp.zeros((8, LANES), jnp.float32)
        padded[c, tiles, own, :] = jnp.zeros((rows, LANES), jnp.float32)
        for j in range(tiles):
            padded[c, j, own, :] = state[c, j, own, :]
    quad = own_applied(padded)
    place = lane_row % SEG

    for i in range(len(rounds)):
        pl.semaphore_wait(round_sem.at[i], 2)
        if i + 1 < len(rounds):
            tell(i + 1)
    for copy in remotes[:stage_one]:
        copy.wait_recv()
    across = jnp.where(place == SEG - 1, pack_one[1] * pltpu.roll(take_one[0], SEG - 1, 1), 0.0)
    across += jnp.where(place == 0, pack_one[0] * pltpu.roll(take_one[1], LANES - SEG + 1, 1), 0.0)
    across = fold(across)
    for c in range(chains):
        along = sum(
            state[c, j, pl.ds(TOP, 1), :] * state[c, j, pl.ds(TOP - 1, 1), :]
            + state[c, j, pl.ds(TOP + rows - 1, 1), :] * state[c, j, pl.ds(TOP + rows, 1), :]
            for j in range(tiles)
        )
        quad[c] = whole(quad[c] - jnp.where(seg % chains == c, across, 0.0) - jnp.where(sublane == 0, along, 0.0))
    send(0, quad, mass)

    for c in range(chains):
        for s in range(fold_one):
            slot = s * chains + c
            part = pl.ds(TOP + s * rows_one, rows_one)
            side = unpack(take_one[0], take_one[1], slot, slot)
            state[c, tiles, part, :] = side
            applied[c, 0, part, :] = applied[c, 0, part, :] - jnp.where(first, pltpu.roll(side, 1, 1), 0.0)
            applied[c, tiles - 1, part, :] = applied[c, tiles - 1, part, :] - jnp.where(
                last, pltpu.roll(side, LANES - 1, 1), 0.0
            )
        for j in range(tiles):
            for here, there in ((TOP, TOP - 1), (TOP + rows - 1, TOP + rows)):
                here, there = pl.ds(here, 1), pl.ds(there, 1)
                applied[c, j, here, :] = applied[c, j, here, :] - state[c, j, there, :]

    xs, ys = weights(0.5)
    mass = own_fresh(xs, ys)

    for copy in early:
        copy.wait_recv()
    for s in range(fold_two):
        for i in range(chains + 2):
            slot = s * (chains + 2) + i
            state[chains + i, tiles, pl.ds(TOP + s * rows_two, rows_two), :] = unpack(
                take_two[0], take_two[1], slot, slot
            )
    for vert, r in ((0, PAD), (1, TOP + rows)):
        for a in range(2 * chains + 2):
            state[a, tiles, pl.ds(r, HALO), :] = unpack(corner_in[0, vert], corner_in[1, vert], a, a)
    def halo_start(regions):
        for r, deep, lane_tiles in regions:
            rowset = pl.ds(r, deep)
            for j in lane_tiles:
                diagonal[j, rowset, :] = state[kap, j, rowset, :] + 4.0
                for c in range(chains):
                    hc = hh[c] * state[cnt, j, rowset, :]
                    scaled[c, j, rowset, :] = hc
                    v = state[c, j, rowset, :]
                    intensity[c, j, rowset, :] = jnp.exp(v)
                    field_u[c, j, rowset, :] = v + (h[c] * state[chains + c, j, rowset, :] + 0.5 * hc)

    halo_start(flanks())
    halo_applied(flanks())
    for c in range(chains):
        x, y = xs[c][:1], ys[c][:1]
        padded[c, tiles, own, :] = (
            field_u[c, tiles, own, :] - x * applied[c, tiles, own, :] - y * intensity[c, tiles, own, :]
        )
        for r in (TOP - 1, TOP + rows):
            line = pl.ds(r, 1)
            cells = [state[c, j, line, :] for j in everything]
            to_right, to_left = [pltpu.roll(z, 1, 1) for z in cells], [pltpu.roll(z, LANES - 1, 1) for z in cells]
            for j in range(tiles):
                beside = jnp.where(first, to_right[(j - 1) % (tiles + 1)], to_right[j])
                beside += jnp.where(last, to_left[j + 1], to_left[j])
                beside += state[c, j, pl.ds(r - 1, 1), :] + state[c, j, pl.ds(r + 1, 1), :]
                av = (state[kap, j, line, :] + 4.0) * cells[j] - beside
                u = cells[j] + (h[c] * state[chains + c, j, line, :] + 0.5 * (hh[c] * state[cnt, j, line, :]))
                padded[c, j, line, :] = u - x * av - y * jnp.exp(cells[j])
        for j in range(tiles):
            padded[c, j, own, :] = fresh[c, j]
    send(1, [whole(q) for q in own_applied(padded)], mass)

    for copy in bulk_rows:
        copy.wait_recv()
    for copy in remotes:
        copy.wait_send()
    halo_start(ends())
    halo_applied(ends())
    halo_advance(xs, ys)
    own_settle()
    halo_applied(sides())
    for r in own_blocks():
        for j, _, value in stencil(state, cnt, r, DEEP, range(tiles)):
            for c in range(chains):
                scaled_applied[c, j, pl.ds(r - TOP, DEEP), :] = hh[c] * value
    for c, sums in own_coefs(True):
        finish_coefs(True, c, sums)

    def step(k, carry):
        kick_hyper(k - 1, jnp.where(k == 1, 0.5, 1.0))
        drift_hyper()
        xs, ys = weights(1.0)
        mass = own_fresh(xs, ys)
        send(k + 1, predicted(xs, ys), mass)
        halo_advance(xs, ys)
        own_settle()
        pairs = list(own_coefs(False))
        halo_applied(sides())
        for c, sums in pairs:
            finish_coefs(False, c, sums)
        return carry

    lax.fori_loop(1, STEPS, step, 0)

    for c in range(chains):
        for j in range(tiles):
            latent_out[c, :, pl.ds(j * LANES, LANES)] = state[c, j, own, :]
    kick_hyper(STEPS - 1, 1.0)
    drift_hyper()
    xs, ys = weights(0.5)
    for c in range(chains):
        x, y = xs[c][:1], ys[c][:1]
        for j in range(tiles):
            moved = field_u[c, j, own, :] - state[c, j, own, :] - 0.5 * scaled[c, j, own, :]
            moved = moved - x * applied[c, j, own, :] - y * intensity[c, j, own, :]
            momentum_out[c, :, pl.ds(j * LANES, LANES)] = moved * (1.0 / full(h[c])[:1])
    out_row, out_col = sublane[:2, :2], lane[:2, :2]

    def show(high, low, ref):
        values = [[scal[base + c][:2, :2] for c in range(chains)] for base in (low, high)]
        pick = [jnp.where(out_col == 0, v[0], v[1]) for v in values]
        ref[...] = jnp.where(out_row == 0, pick[0], pick[1])

    show(HYQ, HYE, hyper_out)
    kick_hyper(STEPS, 0.5)
    show(VEQ, VEE, velocity_out)
    bulk(pl.ds(0, STEPS + 1)).wait_send()


def hand_out(*refs):
    count = (len(refs) - 1) // 2
    sems = refs[-1]
    copies = [pltpu.make_async_copy(refs[i], refs[count + i], sems.at[i]) for i in range(count)]
    for copy in copies:
        copy.start()
    for copy in copies:
        copy.wait()


def solution(mesh):
    nr, nc = mesh.shape["row"], mesh.shape["col"]
    devices = nr * nc

    def shards(latent, momentum, hyper_params, velocity, step_size, counts, kappa_field):
        chains, rows, cols = latent.shape
        tiles = cols // LANES
        deep = rows + 2 * TOP
        total = float(rows * nr * cols * nc)
        sizes = (nr, nc, chains, rows, tiles, total)
        anywhere = pl.BlockSpec(memory_space=pltpu.HBM)
        small = pl.BlockSpec(memory_space=pltpu.VMEM)
        arrays = 2 * chains + 2
        f32 = jnp.float32
        fold_one, fold_two = LANES // (SEG * chains), LANES // (SEG * (chains + 2))
        everywhere = pltpu.VMEM((chains, tiles + 1, deep, LANES), f32)
        inner = pltpu.VMEM((chains, tiles, rows, LANES), f32)
        strip_one = pltpu.VMEM((2, rows // fold_one, LANES), f32)
        strip_two = pltpu.VMEM((2, rows // fold_two, LANES), f32)
        corner = pltpu.VMEM((2, 2, HALO, LANES), f32)
        results = pl.pallas_call(
            functools.partial(kernel, sizes),
            out_shape=(
                jax.ShapeDtypeStruct(latent.shape, f32),
                jax.ShapeDtypeStruct(latent.shape, f32),
                jax.ShapeDtypeStruct(hyper_params.shape, f32),
                jax.ShapeDtypeStruct(velocity.shape, f32),
            ),
            in_specs=[anywhere] * 7,
            out_specs=(small,) * 4,
            scratch_shapes=[
                pltpu.VMEM((arrays, tiles + 1, deep, LANES), f32),
                everywhere,
                pltpu.VMEM((tiles + 1, deep, LANES), f32),
                everywhere,
                everywhere,
                everywhere,
                inner,
                inner,
                pltpu.VMEM((tiles, rows, LANES), jnp.int32),
                everywhere,
                pltpu.VMEM((tiles, rows, LANES), f32),
                strip_one, strip_two, strip_one, strip_two, corner, corner,
                pltpu.VMEM((STEPS + 1, 1, LANES), f32),
                pltpu.VMEM((STEPS + 1, devices, LANES), f32),
                pltpu.VMEM(((6 + COEFS) * chains + 1, 8, LANES), f32),
                pltpu.SMEM(hyper_params.shape, f32),
                pltpu.SMEM(velocity.shape, f32),
                pltpu.SMEM(step_size.shape, f32),
                pltpu.SemaphoreType.DMA((6,)),
                pltpu.SemaphoreType.DMA((16,)),
                pltpu.SemaphoreType.DMA((16,)),
                pltpu.SemaphoreType.DMA,
                pltpu.SemaphoreType.DMA((STEPS + 1,)),
                pltpu.SemaphoreType.REGULAR((len(signal_rounds(nr)),)),
            ],
            compiler_params=pltpu.CompilerParams(
                collective_id=0, has_side_effects=True, vmem_limit_bytes=24 * 1024 * 1024
            ),
        )(*(pltpu.with_memory_space_constraint(x, pltpu.HBM) for x in (
            latent, momentum, counts, kappa_field, hyper_params, velocity, step_size
        )))
        return pl.pallas_call(
            hand_out,
            out_shape=[jax.ShapeDtypeStruct(x.shape, f32) for x in results],
            in_specs=[small] * 4,
            out_specs=[pl.BlockSpec(memory_space=pl.ANY)] * 4,
            scratch_shapes=[pltpu.SemaphoreType.DMA((4,))],
            compiler_params=pltpu.CompilerParams(vmem_limit_bytes=8 * 1024 * 1024),
        )(*results)

    placed = (
        P(None, "row", "col"),
        P(None, "row", "col"),
        P(),
        P(),
        P(),
        P("row", "col"),
        P("row", "col"),
    )
    return jax.shard_map(
        shards,
        mesh=mesh,
        in_specs=placed,
        out_specs=(P(None, "row", "col"), P(None, "row", "col"), P(), P()),
        check_vma=False,
    )
```
